32 devices in a mesh: path: 4 (over z), tm: 8 (over y, x, core).
Axes of the slice: x: 2, y: 2, z: 4, core: 2. Of those that a mesh axis runs over, the one named last changes fastest.
Arguments:
- values: bfloat16 [2048, 16, 2048], P('path', 'tm'), may hold values from -5 to 5
- hazard: float32 [16, 2048], P('tm', 'path'), may hold values from 0.0125 to 0.1875
- spread: float32 [16], P('tm'), may hold values from 0.3 to 3
- trade_set: int32 [2048], replicated, may hold values from 0 to 255
Outputs:
- pathwise_fva: float32 [2048, 256], P(('path', 'tm'))
- set_fva: float32 [256], P(('path', 'tm'))
The draws below stay inside these ranges and needn't reach their ends.
All inputs are finite; a program needn't handle non-finite values.
Results may differ from the reference program's by a relative error of at most 0.0003.
Values sent between devices are 32-bit elements; how exact they have to be, the bound alone decides.
A program may use at most 64 MiB of HBM per device.

```python
import math
import jax
import jax.numpy as jnp
from jax import lax

TRADES = 2048
SETS = 256
PATH_DEV = 512
PATHS = 2048
DATES = 16


def set_ends(result, rng, least, largest):
    extent = result.shape
    place = [jax.random.randint(jax.random.fold_in(rng, axis), (), 0, extent[axis]) for axis in range(len(extent))]
    result = result.at[tuple(place)].set(least)
    longest = extent.index(max(extent))
    place[longest] = (place[longest] + 1) % extent[longest]
    return result.at[tuple(place)].set(largest)


def block_levels(key, dims, shards, smallest, largest):
    gain, own = 1.0, jax.random.fold_in(key, 6)
    for axis_at, blocks in shards:
        draws = jnp.exp(jax.random.uniform(jax.random.fold_in(own, axis_at), (blocks,), jnp.float32, smallest / len(shards), largest / len(shards)))
        gain = gain * jnp.repeat(draws, dims[axis_at] // blocks).reshape([-1 if axis == axis_at else 1 for axis in range(len(dims))])
    return gain


def normal_values(own_key, shape, deviation, bound, shards=(), kind=jnp.bfloat16):
    result = jax.random.normal(own_key, shape, jnp.float32) * deviation
    if len(shards) > 0:
        result = block_levels(own_key, shape, shards, -0.22, 0.18) * result
    return jnp.clip(result, min=-bound, max=bound).astype(kind)


def setup_inputs(seed: int = 0) -> dict:
    keys = jax.random.split(jax.random.key(seed), 5)
    values = normal_values(keys[0], (PATHS, DATES, TRADES), 0.35, 5.0, ((0, 4), (1, 8)))
    hazard = jnp.clip(jnp.exp(math.log(0.1875) - 2.7080502 * jax.random.uniform(keys[1], (DATES, PATHS), jnp.float32) ** block_levels(keys[1], (DATES, PATHS), ((0, 8), (1, 4)), -0.2, 0.2)), 0.0125, 0.1875)
    spread = jnp.clip(jnp.exp(math.log(3.0) - 2.3025851 * jax.random.uniform(keys[2], (DATES,), jnp.float32) ** block_levels(keys[2], (DATES,), ((0, 8),), -0.2, 0.2)), 0.3, 3.0)
    trade_set = set_ends(jax.random.randint(keys[3], (TRADES,), 0, SETS), jax.random.fold_in(keys[3], 1), 0, SETS - 1).astype(jnp.int32)
    return dict(values=values, hazard=hazard, spread=spread, trade_set=trade_set)


def reference(values, hazard, spread, trade_set):
    onehot = (trade_set[:, None] == jnp.arange(SETS, dtype=jnp.int32)[None, :]).astype(jnp.bfloat16)
    survival = jnp.exp(-jnp.cumsum(hazard, axis=0))
    weights = spread[:, None] * survival
    blocks = PATHS // PATH_DEV
    value_blocks = values.reshape(blocks, PATH_DEV, DATES, TRADES)
    weight_blocks = jnp.transpose(weights.reshape(DATES, blocks, PATH_DEV), (1, 2, 0))

    def one_block(item):
        block_values, block_weights = item
        netted = jnp.dot(block_values.reshape(PATH_DEV * DATES, TRADES), onehot, preferred_element_type=jnp.float32)
        positive = jnp.maximum(netted.reshape(PATH_DEV, DATES, SETS), 0.0)
        return jnp.einsum("pt,pts->ps", block_weights, positive, precision=lax.Precision.HIGHEST)

    pathwise_fva = lax.map(one_block, (value_blocks, weight_blocks)).reshape(PATHS, SETS) / DATES
    set_fva = jnp.sum(pathwise_fva, axis=0) / PATHS
    return pathwise_fva, set_fva
```

```python
import functools

import jax
import jax.numpy as jnp
from jax import lax
from jax.experimental import pallas as pl
from jax.experimental.pallas import tpu as pltpu
from jax.sharding import PartitionSpec as P

SETS = 256
CHUNK_PATHS = 128
LANES = 128
PACK = 16
BARRIER_AFTER = 0
MESH = pl.DeviceIdType.MESH
DOT_NT = (((1,), (1,)), ((), ()))


def kernel(
    n_path, n_tm, values, hazard_in, spread_in, trade_in, out, set_out,
    vbuf, ts, oh, hz, spread, nbuf, wt, contrib, pair, comb, recv, bsum, hbuf, pcol, ecol, row_a, rows_a,
    load_sem, small_sem, h_send, hp_recv, h_recv, p_send, p_recv, b_send, b_recv, a_send, a_recv, ready,
):
    paths, dates, trades = values.shape
    f32, bf16 = jnp.float32, jnp.bfloat16
    own = paths // n_tm
    chunks = paths // CHUNK_PATHS
    per = n_tm // chunks
    n_all = n_path * n_tm
    chips = n_tm // 2
    share = SETS // n_all
    path_at, me = lax.axis_index("path"), lax.axis_index("tm")
    flat = path_at * n_tm + me
    chip, core = lax.div(me, 2), lax.rem(me, 2)
    partner = me + 1 - 2 * core
    peers = [lax.rem(me + k, n_tm) for k in range(1, n_tm)]
    path_peers = [lax.rem(path_at + k, n_path) for k in range(1, n_path)]
    rows = CHUNK_PATHS * dates
    my_chunk = lax.div(me, per)
    if chunks == 4:
        high, low = lax.div(my_chunk, 2), lax.rem(my_chunk, 2)
        first = [2 * (1 - high) + 1 - low, 2 * high + 1 - low, 2 * (1 - high) + low, my_chunk]
    else:
        first = [lax.rem(my_chunk + 1 + i, chunks) for i in range(chunks)]
    flat_values = values.reshape(paths * dates, trades)

    def load(i):
        span = pl.ds(pl.multiple_of(first[i] * rows, rows), rows)
        return pltpu.make_async_copy(flat_values.at[span], vbuf.at[span], load_sem.at[i])

    copy_trades = pltpu.make_async_copy(trade_in, ts, small_sem.at[0])
    copy_hazard = pltpu.make_async_copy(hazard_in, hz, small_sem.at[1])
    copy_spread = pltpu.make_async_copy(spread_in, spread, small_sem.at[2])
    copy_trades.start()
    copy_hazard.start()
    copy_spread.start()
    for i in range(chunks):
        load(i).start()

    barrier = pltpu.get_barrier_semaphore()
    for other in peers:
        pl.semaphore_signal(barrier, inc=1, device_id=(path_at, other), device_id_type=MESH)
    for other in path_peers:
        pl.semaphore_signal(barrier, inc=1, device_id=(other, me), device_id_type=MESH)

    def remote(src, dst, send, recv_at, device):
        return pltpu.make_async_remote_copy(
            src_ref=src, dst_ref=dst, send_sem=send, recv_sem=recv_at, device_id=device, device_id_type=MESH
        )

    def own_rows(index):
        return pl.ds(pl.multiple_of(index * own, own), own)

    def hazard_copy(other, arrival):
        return remote(bsum, hbuf.at[me], h_send, arrival, (path_at, other))

    def hazards(count, send, arrival):
        span = hbuf.at[pl.ds(0, count)]
        return remote(span, span, send, arrival, (path_at, partner))

    def pair_copy(q):
        theirs = contrib.at[own_rows(q * 2 + 1 - core)]
        return remote(theirs, pair.at[q], p_send, p_recv.at[q], (path_at, partner))

    def block_copy(q, slot):
        return remote(comb.at[q], recv.at[slot], b_send, b_recv.at[slot], (path_at, q * 2 + core))

    targets = [(z, other) for z in path_peers for other in [me] + peers]
    targets += [(path_at, other) for other in peers]

    def set_row(z, other):
        half = lax.div((z * n_tm + other) * share, LANES)
        return remote(row_a.at[half], rows_a.at[flat], a_send, a_recv, (z, other))

    copy_trades.wait()
    base = lax.broadcasted_iota(jnp.int32, (PACK, LANES), 0)
    set_at = [(base + PACK * r).astype(f32).astype(bf16) for r in range(SETS // PACK)]
    one, zero = jnp.ones((PACK, LANES), bf16), jnp.zeros((PACK, LANES), bf16)
    for block in range(trades // LANES):
        ids = jnp.broadcast_to(ts[pl.ds(block, 1), :], (PACK, LANES)).astype(f32).astype(bf16)
        for r in range(SETS // PACK):
            picked = jnp.where(ids == set_at[r], one, zero)
            oh[pl.ds(r * PACK, PACK), pl.ds(block * LANES, LANES)] = picked.astype(oh.dtype)

    copy_hazard.wait()
    copy_spread.wait()
    total = jnp.zeros((1, paths), f32)
    weight_rows = []
    scale = 1.0 / (dates * n_tm)
    for d in range(dates):
        total = total + hz[pl.ds(d, 1), :]
        weight_rows.append((spread[d] * scale) * jnp.exp(-total))
    weight_rows.append(jnp.zeros((8 - dates, paths), f32))
    wt[...] = jnp.transpose(jnp.concatenate(weight_rows, axis=0))
    bsum[...] = total
    hbuf[me] = total

    def meet():
        pl.semaphore_wait(barrier, n_tm - 1 + n_path - 1)
        hazard_copy(partner, hp_recv).start()
        for other in peers:
            @pl.when(other != partner)
            def _():
                hazard_copy(other, h_recv).start()
        for other in path_peers:
            pl.semaphore_signal(ready, inc=1, device_id=(other, me), device_id_type=MESH)

    def exchange(i):
        for k in range(per // 2):
            pair_copy(first[i] * (per // 2) + k).start()

    def combine(q):
        remote(pair.at[q], pair.at[q], p_send, p_recv.at[q], (path_at, partner)).wait_recv()
        mine = own_rows(q * 2 + core)
        factor = pcol[mine, :]
        return factor[:, 0:1] * contrib[mine, :] + factor[:, 1:2] * pair[q]

    def forward(i):
        for k in range(per // 2):
            q = first[i] * (per // 2) + k
            comb[q] = combine(q)
            block_copy(q, chip).start()

    if BARRIER_AFTER < 0:
        meet()
    for i in range(chunks):
        load(i).wait()
        half_rows = rows // 2
        for k in range(2):
            begin = pl.multiple_of(first[i] * rows + k * half_rows, half_rows)
            netted = lax.dot_general(
                vbuf[pl.ds(begin, half_rows), :], oh[...], DOT_NT, preferred_element_type=f32
            )
            for h in range(SETS // LANES):
                nbuf[i, h, pl.ds(k * half_rows, half_rows)] = netted[:, h * LANES : (h + 1) * LANES]
        path_span = pl.ds(pl.multiple_of(first[i] * CHUNK_PATHS, CHUNK_PATHS), CHUNK_PATHS)
        weight = wt[path_span, :]
        for h in range(SETS // LANES):
            part = None
            for d in range(dates):
                picked = nbuf[i, h, pl.ds(d, CHUNK_PATHS, stride=dates), :]
                term = weight[:, d : d + 1] * jnp.maximum(picked, 0.0)
                part = term if part is None else part + term
            contrib[path_span, pl.ds(h * LANES, LANES)] = part
        if i == BARRIER_AFTER:
            meet()
        if i >= BARRIER_AFTER:
            for j in range(i + 1 if i == BARRIER_AFTER else 1):
                exchange(i if i != BARRIER_AFTER else j)

    hazards(1, h_send, hp_recv).wait_recv()
    block = hbuf[me - core]
    late = core.astype(f32)
    factors = [jnp.exp(-late * block), jnp.exp((late - 1.0) * block)]
    factors.append(jnp.zeros((6, paths), f32))
    pcol[...] = jnp.transpose(jnp.concatenate(factors, axis=0))
    for i in range(chunks - 2):
        forward(i)

    hazards(n_tm - 2, h_send, h_recv).wait_recv()
    before = jnp.zeros((1, paths), f32)
    for k in range(n_tm - 1):
        before = before + jnp.where(k < me, hbuf[k], 0.0)
    column = jnp.transpose(jnp.broadcast_to(jnp.exp(-before), (8, paths)))[:, 0:1]
    factor = jnp.broadcast_to(column, (paths, LANES))
    for h in range(SETS // LANES):
        part = jnp.sum(factor * contrib[:, pl.ds(h * LANES, LANES)], axis=0, keepdims=True)
        row_a[h] = part * (1.0 / (paths * n_path))
    pl.semaphore_wait(ready, n_path - 1)
    for z, other in targets:
        set_row(z, other).start()
    forward(chunks - 2)
    own_chips = [my_chunk * (per // 2) + lax.rem(lax.rem(chip, per // 2) + k, per // 2) for k in range(per // 2)]
    for q in own_chips[1:]:
        comb[q] = combine(q)
        block_copy(q, chip).start()
    my_half = lax.div(flat * share, LANES)
    rows_a[flat] = row_a[my_half]
    before = jnp.zeros((1, paths), f32)
    prefix = []
    for k in range(n_tm):
        prefix.append(before)
        before = before + hbuf[k]
    ecol[...] = jnp.transpose(jnp.exp(-jnp.concatenate(prefix, axis=0)))
    factor = ecol[own_rows(me), :]
    recv[chip] = combine(own_chips[0])

    other_chips = [lax.rem(chip + k, chips) for k in range(1, chips)]
    for q in other_chips:
        remote(recv.at[q], recv.at[q], b_send, b_recv.at[q], (path_at, me)).wait_recv()
    result = None
    for k in range(chips):
        term = factor[:, 2 * k : 2 * k + 1] * recv[k]
        result = term if result is None else result + term
    out[...] = result

    span = rows_a.at[pl.ds(0, n_all - 1)]
    arrived = remote(span, span, a_send, a_recv, (path_at, partner))
    arrived.wait_recv()
    sums = jnp.broadcast_to(jnp.sum(rows_a[...], axis=0), (8, LANES))
    turned = pltpu.roll(sums, lax.rem(LANES - (flat * share - my_half * LANES), LANES), 1)
    set_out[...] = turned[:1, :share]

    arrived.wait_send()
    hazards(n_tm - 1, h_send, h_recv).wait_send()
    span = recv.at[pl.ds(0, chips - 1)]
    remote(span, span, b_send, b_recv.at[0], (path_at, partner)).wait_send()
    remote(pair, pair, p_send, p_recv.at[0], (path_at, partner)).wait_send()


def finish(pathwise, sets, pathwise_out, sets_out, sem):
    copies = [
        pltpu.make_async_copy(pathwise, pathwise_out, sem.at[0]),
        pltpu.make_async_copy(sets, sets_out, sem.at[1]),
    ]
    for copy in copies:
        copy.start()
    for copy in copies:
        copy.wait()


def solution(mesh):
    n_path, n_tm = mesh.shape["path"], mesh.shape["tm"]
    n_all = n_path * n_tm

    def on_device(values, hazard, spread, trade_set):
        paths, dates, trades = values.shape
        own = paths // n_tm
        chunks = paths // CHUNK_PATHS
        f32 = jnp.float32
        hbm = pl.BlockSpec(memory_space=pltpu.HBM)
        vmem = pl.BlockSpec(memory_space=pltpu.VMEM)
        dma = pltpu.SemaphoreType.DMA
        pathwise, sets = pl.pallas_call(
            functools.partial(kernel, n_path, n_tm),
            out_shape=(pltpu.VMEM((own, SETS), f32), pltpu.VMEM((1, SETS // n_all), f32)),
            in_specs=[hbm, hbm, hbm, hbm],
            out_specs=(vmem, vmem),
            scratch_shapes=[
                pltpu.VMEM((paths * dates, trades), jnp.bfloat16),
                pltpu.VMEM((trades // LANES, LANES), jnp.int32),
                pltpu.VMEM((SETS, trades), jnp.float8_e4m3fn),
                pltpu.VMEM((dates, paths), f32),
                pltpu.SMEM((dates,), f32),
                pltpu.VMEM((chunks, SETS // LANES, CHUNK_PATHS * dates, LANES), f32),
                pltpu.VMEM((paths, 8), f32),
                pltpu.VMEM((paths, SETS), f32),
                pltpu.VMEM((n_tm // 2, own, SETS), f32),
                pltpu.VMEM((n_tm // 2, own, SETS), f32),
                pltpu.VMEM((n_tm // 2, own, SETS), f32),
                pltpu.VMEM((1, paths), f32),
                pltpu.VMEM((n_tm, 1, paths), f32),
                pltpu.VMEM((paths, 8), f32),
                pltpu.VMEM((paths, n_tm), f32),
                pltpu.VMEM((SETS // LANES, 1, LANES), f32),
                pltpu.VMEM((n_all, 1, LANES), f32),
                dma((chunks,)),
                dma((3,)),
                dma,
                dma,
                dma,
                dma,
                dma((n_tm // 2,)),
                dma,
                dma((n_tm // 2,)),
                dma,
                dma,
                pltpu.SemaphoreType.REGULAR,
            ],
            compiler_params=pltpu.CompilerParams(
                collective_id=0, has_side_effects=True, vmem_limit_bytes=62 * 1024 * 1024
            ),
        )(values, hazard, spread, trade_set.reshape(trades // LANES, LANES))
        pathwise = pltpu.with_memory_space_constraint(pathwise, pltpu.VMEM)
        sets = pltpu.with_memory_space_constraint(sets, pltpu.VMEM)
        pathwise, sets = pl.pallas_call(
            finish,
            out_shape=(
                jax.ShapeDtypeStruct(pathwise.shape, f32),
                jax.ShapeDtypeStruct(sets.shape, f32),
            ),
            in_specs=[vmem, vmem],
            out_specs=(hbm, hbm),
            scratch_shapes=[dma((2,))],
        )(pathwise, sets)
        return pathwise, sets.reshape(SETS // n_all)

    in_specs = (P("path", "tm", None), P("tm", "path"), P("tm"), P())
    out_specs = (P(("path", "tm"), None), P(("path", "tm")))
    return jax.shard_map(
        on_device, mesh=mesh, in_specs=in_specs, out_specs=out_specs, check_vma=False
    )
```

```python
import functools

import jax
import jax.numpy as jnp
from jax import lax
from jax.experimental import pallas as pl
from jax.experimental.pallas import tpu as pltpu
from jax.sharding import PartitionSpec as P

SETS = 256
CHUNK_PATHS = 128
LANES = 128
PACK = 16
TILE = 256
BARRIER_AFTER = 0
MESH = pl.DeviceIdType.MESH


def kernel(n_path, n_tm, *refs):
    rows = CHUNK_PATHS * refs[0].shape[1]
    sums = [pltpu.ACC(unit)((rows, SETS), jnp.float32) for unit in (0, 0, 1, 1)]
    sums += [pltpu.ACC(unit)((PACK, SETS), jnp.float32) for unit in (0, 1)]
    pl.run_scoped(lambda *totals: body(n_path, n_tm, totals, *refs), *sums)


def body(
    n_path, n_tm, totals, values, hazard_in, spread_in, trade_in, out, set_out,
    vbuf, ts, oh, hz, spread, nbuf, wt, contrib, theirs, comb, recv, bsum, before_me, hbuf, pcol, ecol, limbs, row_a, rows_a,
    load_sem, small_sem, h_send, h_recv, p_send, p_recv, b_send, b_recv, a_send, a_recv, ready, above,
):
    paths, dates, trades = values.shape
    f32, bf16 = jnp.float32, jnp.bfloat16
    own = paths // n_tm
    chunks = paths // CHUNK_PATHS
    per = n_tm // chunks
    n_all = n_path * n_tm
    chips = n_tm // 2
    share = SETS // n_all
    path_at, me = lax.axis_index("path"), lax.axis_index("tm")
    flat = path_at * n_tm + me
    chip, core = lax.div(me, 2), lax.rem(me, 2)
    partner = me + 1 - 2 * core
    peers = [lax.rem(me + k, n_tm) for k in range(1, n_tm)]
    leads = core == 1
    senders = n_path * chips
    slot = path_at * chips + chip
    rows = CHUNK_PATHS * dates
    my_chunk = lax.div(me, per)
    if chunks == 4:
        high, low = lax.div(my_chunk, 2), lax.rem(my_chunk, 2)
        first = [2 * (1 - high) + 1 - low, 2 * high + 1 - low, 2 * (1 - high) + low, my_chunk]
    else:
        first = [lax.rem(my_chunk + 1 + i, chunks) for i in range(chunks)]
    flat_values = values.reshape(paths * dates, trades)

    def load(i):
        span = pl.ds(pl.multiple_of(first[i] * rows, rows), rows)
        return pltpu.make_async_copy(flat_values.at[span], vbuf.at[span], load_sem.at[i])

    barrier = pltpu.get_barrier_semaphore()
    for other in peers:
        pl.semaphore_signal(barrier, inc=1, device_id=(path_at, other), device_id_type=MESH)

    copy_trades = pltpu.make_async_copy(trade_in, ts, small_sem.at[0])
    copy_hazard = pltpu.make_async_copy(hazard_in, hz, small_sem.at[1])
    copy_spread = pltpu.make_async_copy(spread_in, spread, small_sem.at[2])
    copy_trades.start()
    copy_hazard.start()
    copy_spread.start()
    for i in range(chunks):
        load(i).start()
    for z in range(1, n_path):
        @pl.when(z > path_at)
        def _():
            pl.semaphore_signal(barrier, inc=1, device_id=(z, me), device_id_type=MESH)

    def remote(src, dst, send, recv_at, device):
        return pltpu.make_async_remote_copy(
            src_ref=src, dst_ref=dst, send_sem=send, recv_sem=recv_at, device_id=device, device_id_type=MESH
        )

    def chunk_span(i):
        return pl.ds(pl.multiple_of(first[i] * CHUNK_PATHS, CHUNK_PATHS), CHUNK_PATHS)

    def own_rows(index):
        return pl.ds(pl.multiple_of(index * own, own), own)

    def hazard_copy(other, arrival):
        return remote(bsum, hbuf.at[me], h_send, h_recv.at[arrival], (path_at, other))

    def hazards(count, arrival):
        span = hbuf.at[pl.ds(0, count)]
        return remote(span, span, h_send, h_recv.at[arrival], (path_at, partner))

    def from_chips(arrival, chips_there):
        for c in range(1, chips):
            @pl.when(chips_there == c)
            def _():
                hazards(2 * c, arrival).wait_recv()

    def both_rows(q):
        return pl.ds(pl.multiple_of(q * 2 * own, 2 * own), 2 * own)

    def pair_copy(q, span):
        return remote(contrib.at[span], theirs.at[span], p_send, p_recv.at[q], (path_at, partner))

    def per_core(q, act):
        @pl.when(leads)
        def _():
            act(q, own_rows(q * 2), both_rows(q))

        @pl.when(jnp.logical_not(leads))
        def _():
            act(q, both_rows(q), own_rows(q * 2))

    def block_copy(q, slot_at):
        return remote(comb.at[own_rows(q * 2 + core)], recv.at[slot_at], b_send, b_recv, (path_at, q * 2 + core))

    def set_row(z, other):
        half = lax.div((z * n_tm + other) * share, LANES)
        return remote(row_a.at[half], rows_a.at[slot], a_send, a_recv, (z, other))

    def set_rows(count):
        span = rows_a.at[pl.ds(0, count)]
        return remote(span, span, a_send, a_recv, (path_at, partner))

    copy_trades.wait()
    base = lax.broadcasted_iota(jnp.int32, (PACK, LANES), 0)
    set_at = [(base + PACK * r).astype(f32).astype(bf16) for r in range(SETS // PACK)]
    one, zero = jnp.ones((PACK, LANES), bf16), jnp.zeros((PACK, LANES), bf16)
    for block in range(trades // LANES):
        ids = jnp.broadcast_to(ts[pl.ds(block, 1), :], (PACK, LANES)).astype(f32).astype(bf16)
        for r in range(SETS // PACK):
            picked = jnp.where(ids == set_at[r], one, zero)
            oh[pl.ds(r * PACK, PACK), pl.ds(block * LANES, LANES)] = picked.astype(oh.dtype)

    copy_hazard.wait()
    copy_spread.wait()
    total = jnp.zeros((1, paths), f32)
    weight_rows = []
    scale = 1.0 / (dates * n_tm)
    for d in range(dates):
        total = total + hz[pl.ds(d, 1), :]
        weight_rows.append((spread[d] * scale) * jnp.exp(-total))
    weight_rows.append(jnp.zeros((8 - dates, paths), f32))
    wt[...] = jnp.transpose(jnp.concatenate(weight_rows, axis=0))
    bsum[...] = total
    hbuf[me] = total

    def meet():
        pl.semaphore_wait(barrier, n_tm - 1 + path_at)
        hazard_copy(partner, 0).start()
        for side in (1, 0):
            for k in range(1, chips):
                there = lax.rem(chip + k, chips)
                hazard_copy(there * 2 + side, jnp.where(there > chip, 1, 2)).start()
        for k in range(chips):
            @pl.when(jnp.logical_or(jnp.logical_not(leads), k > 0))
            def _():
                other = lax.rem(chip + k, chips) * 2 + 1
                pl.semaphore_signal(ready, inc=1, device_id=(path_at, other), device_id_type=MESH)
        for z in range(n_path - 1):
            @pl.when(jnp.logical_and(leads, z < path_at))
            def _():
                pl.semaphore_signal(above, inc=1, device_id=(z, me), device_id_type=MESH)

    def exchange(i):
        for k in range(per // 2):
            per_core(first[i] * (per // 2) + k, lambda q, send, take: pair_copy(q, send).start())

    def combine(q):
        per_core(q, lambda q, send, take: pair_copy(q, take).wait_recv())

        @pl.when(leads)
        def _():
            span = both_rows(q)
            both = theirs[span, :] + pcol[span, 0:1] * contrib[span, :]
            comb[span, :] = both
            upper = both.astype(bf16)
            limbs[0, span, :] = upper
            limbs[1, span, :] = (both - upper.astype(f32)).astype(bf16)

        @pl.when(jnp.logical_not(leads))
        def _():
            span = own_rows(q * 2)
            comb[span, :] = contrib[span, :] + pcol[span, 0:1] * theirs[span, :]

    own_chips = [my_chunk * (per // 2) + lax.rem(lax.rem(chip, per // 2) + k, per // 2) for k in range(per // 2)]
    other_chips = [first[i] * (per // 2) + k for i in range(chunks - 1) for k in range(per // 2)]
    other_chips += own_chips[1:]

    tiles = trades // TILE // 2

    def multiply(i):
        span = pl.ds(pl.multiple_of(first[i] * rows, rows), rows)
        for t in range(tiles):
            for unit in range(2):
                ids = oh[:, pl.ds((unit * tiles + t) * TILE, TILE)]
                pltpu.matmul_push_rhs(ids, staging_register=t % 2, mxu_index=unit, transpose=True)
            for unit in range(2):
                block = vbuf[span, pl.ds((unit * tiles + t) * TILE, TILE)]
                pltpu.matmul_acc_lhs(totals[unit * 2 + i % 2], block, load_staged_rhs=t % 2)

    def weigh(i):
        netted = pltpu.matmul_pop(totals[i % 2]) + pltpu.matmul_pop(totals[2 + i % 2])
        for h in range(SETS // LANES):
            nbuf[i, h] = netted[:, h * LANES : (h + 1) * LANES]
        path_span = chunk_span(i)
        weight = wt[path_span, :]
        for h in range(SETS // LANES):
            part = None
            for d in range(dates):
                picked = nbuf[i, h, pl.ds(d, CHUNK_PATHS, stride=dates), :]
                term = weight[:, d : d + 1] * jnp.maximum(picked, 0.0)
                part = term if part is None else part + term
            contrib[path_span, pl.ds(h * LANES, LANES)] = part

    if BARRIER_AFTER < 0:
        meet()
    for i in range(chunks):
        load(i).wait()
        if i > 0:
            weigh(i - 1)
        multiply(i)
        if i == BARRIER_AFTER:
            meet()
        if i > 0 and i >= BARRIER_AFTER:
            for j in range(0 if i == BARRIER_AFTER else i - 1, i):
                exchange(j)
    weigh(chunks - 1)
    exchange(chunks - 1)

    @pl.when(leads)
    def _():
        hazards(1, 0).wait_recv()
    block = jnp.broadcast_to(jnp.exp(-hbuf[me - core]), (8, paths))
    pcol[...] = jnp.transpose(block)
    for q in other_chips:
        combine(q)

        @pl.when(jnp.logical_not(leads))
        def _():
            block_copy(q, chip).start()

    combine(own_chips[0])

    def limb(unit, t, part):
        block = limbs[part, pl.ds((unit * row_tiles + t) * TILE, TILE), :]
        pltpu.matmul_push_rhs(block, staging_register=part, mxu_index=unit)

    row_tiles = paths // TILE // 2
    @pl.when(leads)
    def _():
        for unit in range(2):
            for part in range(2):
                limb(unit, 0, part)
        from_chips(1, chip)
        before_me[...] = jnp.zeros((1, paths), f32)
        for c in range(1, chips):
            @pl.when(chip == c)
            def _():
                before_me[...] = sum(hbuf[k] for k in range(2 * c))
        earlier = jnp.broadcast_to(jnp.exp(-before_me[...]), (PACK, paths))
        upper = earlier.astype(bf16).astype(f32)
        at = lax.broadcasted_iota(jnp.int32, (PACK, paths), 0)
        weights = jnp.where(at == 0, upper, jnp.where(at == 1, earlier - upper, 0.0)).astype(bf16)
        for t in range(row_tiles):
            for unit in range(2):
                if t > 0:
                    limb(unit, t, 0)
                    limb(unit, t, 1)
                begin = (unit * row_tiles + t) * TILE
                for part in range(2):
                    pltpu.matmul_acc_lhs(totals[4 + unit], weights[:, begin : begin + TILE], load_staged_rhs=part)
        both = pltpu.matmul_pop(totals[4]) + pltpu.matmul_pop(totals[5])
        line = (both[0:1] + both[1:2]) * (1.0 / (paths * n_path))
        for h in range(SETS // LANES):
            row_a[h] = line[:, h * LANES : (h + 1) * LANES]
        pl.semaphore_wait(ready, n_tm - 1)
        for z in range(n_path - 1):
            @pl.when(z < path_at)
            def _():
                for k in range(n_tm):
                    set_row(z, lax.rem(me + 1 + k, n_tm)).start()
        for other in peers:
            set_row(path_at, other).start()

        @pl.when(path_at < n_path - 1)
        def _():
            pl.semaphore_wait(above, n_path - 1 - path_at)
        for z in range(1, n_path):
            @pl.when(z > path_at)
            def _():
                for k in range(n_tm):
                    set_row(z, lax.rem(me + 1 + k, n_tm)).start()
        for q in other_chips:
            block_copy(q, chip).start()
        rows_a[slot] = row_a[lax.div(flat * share, LANES)]

    from_chips(2, chips - 1 - chip)

    @pl.when(jnp.logical_not(leads))
    def _():
        hazards(1, 0).wait_recv()
        from_chips(1, chip)
    before = jnp.zeros((1, paths), f32)
    prefix = []
    for k in range(n_tm):
        if k % 2 == 0:
            prefix.append(before)
        before = before + hbuf[k]
    if chips < 8:
        prefix.append(jnp.zeros((8 - chips, paths), f32))
    ecol[...] = jnp.transpose(jnp.exp(-jnp.concatenate(prefix, axis=0)))
    factor = ecol[own_rows(me), :]
    recv[chip] = comb[own_rows(me), :]

    span = recv.at[pl.ds(0, chips - 1)]
    blocks = remote(span, span, b_send, b_recv, (path_at, partner))
    blocks.wait_recv()
    result = None
    for k in range(chips):
        term = factor[:, k : k + 1] * recv[k]
        result = term if result is None else result + term
    out[...] = result

    @pl.when(leads)
    def _():
        set_rows(senders - 1).wait_recv()

    @pl.when(jnp.logical_not(leads))
    def _():
        set_rows(senders).wait_recv()
    sums = jnp.broadcast_to(jnp.sum(rows_a[...], axis=0), (8, LANES))
    turned = pltpu.roll(sums, lax.rem(LANES - lax.rem(flat * share, LANES), LANES), 1)
    set_out[...] = turned[:1, :share]

    span = hbuf.at[pl.ds(0, n_tm - 1)]
    remote(span, span, h_send, h_recv.at[0], (path_at, partner)).wait_send()
    blocks.wait_send()

    @pl.when(leads)
    def _():
        span = rows_a.at[pl.ds(0, senders - 1)]
        sent = remote(span, span, a_send, a_recv, (path_at, partner))
        sent.wait_send()
        span = rows_a.at[pl.ds(0, senders)]
        sent = remote(span, span, a_send, a_recv, (path_at, partner))
        sent.wait_send()
        span = theirs.at[pl.ds(0, paths // 2)]
        remote(span, span, p_send, p_recv.at[0], (path_at, partner)).wait_send()

    @pl.when(jnp.logical_not(leads))
    def _():
        remote(theirs, theirs, p_send, p_recv.at[0], (path_at, partner)).wait_send()


def finish(pathwise, sets, pathwise_out, sets_out, sem):
    copies = [
        pltpu.make_async_copy(pathwise, pathwise_out, sem.at[0]),
        pltpu.make_async_copy(sets, sets_out, sem.at[1]),
    ]
    for copy in copies:
        copy.start()
    for copy in copies:
        copy.wait()


def solution(mesh):
    n_path, n_tm = mesh.shape["path"], mesh.shape["tm"]
    n_all = n_path * n_tm

    def on_device(values, hazard, spread, trade_set):
        paths, dates, trades = values.shape
        own = paths // n_tm
        chunks = paths // CHUNK_PATHS
        f32 = jnp.float32
        hbm = pl.BlockSpec(memory_space=pltpu.HBM)
        vmem = pl.BlockSpec(memory_space=pltpu.VMEM)
        dma = pltpu.SemaphoreType.DMA
        pathwise, sets = pl.pallas_call(
            functools.partial(kernel, n_path, n_tm),
            out_shape=(pltpu.VMEM((own, SETS), f32), pltpu.VMEM((1, SETS // n_all), f32)),
            in_specs=[hbm, hbm, hbm, hbm],
            out_specs=(vmem, vmem),
            scratch_shapes=[
                pltpu.VMEM((paths * dates, trades), jnp.bfloat16),
                pltpu.VMEM((trades // LANES, LANES), jnp.int32),
                pltpu.VMEM((SETS, trades), jnp.float8_e4m3fn),
                pltpu.VMEM((dates, paths), f32),
                pltpu.SMEM((dates,), f32),
                pltpu.VMEM((chunks, SETS // LANES, CHUNK_PATHS * dates, LANES), f32),
                pltpu.VMEM((paths, 8), f32),
                pltpu.VMEM((paths, SETS), f32),
                pltpu.VMEM((paths, SETS), f32),
                pltpu.VMEM((paths, SETS), f32),
                pltpu.VMEM((n_tm // 2, own, SETS), f32),
                pltpu.VMEM((1, paths), f32),
                pltpu.VMEM((1, paths), f32),
                pltpu.VMEM((n_tm, 1, paths), f32),
                pltpu.VMEM((paths, 8), f32),
                pltpu.VMEM((paths, max(8, n_tm // 2)), f32),
                pltpu.VMEM((2, paths, SETS), jnp.bfloat16),
                pltpu.VMEM((SETS // LANES, 1, LANES), f32),
                pltpu.VMEM((n_all // 2, 1, LANES), f32),
                dma((chunks,)),
                dma((3,)),
                dma,
                dma((3,)),
                dma,
                dma((n_tm // 2,)),
                dma,
                dma,
                dma,
                dma,
                pltpu.SemaphoreType.REGULAR,
                pltpu.SemaphoreType.REGULAR,
            ],
            compiler_params=pltpu.CompilerParams(
                collective_id=0, has_side_effects=True, vmem_limit_bytes=62 * 1024 * 1024
            ),
        )(values, hazard, spread, trade_set.reshape(trades // LANES, LANES))
        pathwise = pltpu.with_memory_space_constraint(pathwise, pltpu.VMEM)
        sets = pltpu.with_memory_space_constraint(sets, pltpu.VMEM)
        pathwise, sets = pl.pallas_call(
            finish,
            out_shape=(
                jax.ShapeDtypeStruct(pathwise.shape, f32),
                jax.ShapeDtypeStruct(sets.shape, f32),
            ),
            in_specs=[vmem, vmem],
            out_specs=(hbm, hbm),
            scratch_shapes=[dma((2,))],
        )(pathwise, sets)
        return pathwise, sets.reshape(SETS // n_all)

    in_specs = (P("path", "tm", None), P("tm", "path"), P("tm"), P())
    out_specs = (P(("path", "tm"), None), P(("path", "tm")))
    return jax.shard_map(
        on_device, mesh=mesh, in_specs=in_specs, out_specs=out_specs, check_vma=False
    )
```

```python
import functools

import jax
import jax.numpy as jnp
from jax import lax
from jax.experimental import pallas as pl
from jax.experimental.pallas import tpu as pltpu
from jax.sharding import PartitionSpec as P

SETS = 256
CHUNK_PATHS = 128
LANES = 128
PACK = 16
TILE = 256
BARRIER_AFTER = 1
MESH = pl.DeviceIdType.MESH


def kernel(n_path, n_tm, *refs):
    rows = CHUNK_PATHS * refs[0].shape[1]
    sums = [pltpu.ACC(unit)((rows, SETS), jnp.float32) for unit in (0, 0, 1, 1)]
    sums += [pltpu.ACC(unit)((PACK, SETS), jnp.float32) for unit in (0, 1)]
    pl.run_scoped(lambda *totals: body(n_path, n_tm, totals, *refs), *sums)


def body(
    n_path, n_tm, totals, values, hazard_in, spread_in, trade_in, out, set_out,
    vbuf, ts, oh, hz, spread, nbuf, wt, contrib, theirs, comb, recv, bsum, mate_sum, before_me, hbuf, pcol, ecol, limbs, row_a, rows_a,
    load_sem, small_sem, h_send, h_recv, p_send, p_recv, b_send, b_recv, a_send, a_recv, mate, ready, above,
):
    paths, dates, trades = values.shape
    f32, bf16 = jnp.float32, jnp.bfloat16
    own = paths // n_tm
    chunks = paths // CHUNK_PATHS
    per = n_tm // chunks
    n_all = n_path * n_tm
    chips = n_tm // 2
    share = SETS // n_all
    path_at, me = lax.axis_index("path"), lax.axis_index("tm")
    flat = path_at * n_tm + me
    chip, core = lax.div(me, 2), lax.rem(me, 2)
    partner = me + 1 - 2 * core
    peers = [lax.rem(me + k, n_tm) for k in range(1, n_tm)]
    leads = core == 1
    lead_peers = [lax.rem(chip + k, chips) * 2 + 1 for k in range(1, chips)]
    senders = n_path * chips
    slot = path_at * chips + chip
    rows = CHUNK_PATHS * dates
    my_chunk = lax.div(me, per)
    if chunks == 4:
        high, low = lax.div(my_chunk, 2), lax.rem(my_chunk, 2)
        first = [2 * (1 - high) + 1 - low, 2 * high + 1 - low, 2 * (1 - high) + low, my_chunk]
    else:
        first = [lax.rem(my_chunk + 1 + i, chunks) for i in range(chunks)]
    flat_values = values.reshape(paths * dates, trades)

    half = trades // 2
    halved = tuple(range(chunks))

    def load(i, part):
        span = pl.ds(pl.multiple_of(first[i] * rows, rows), rows)
        at = i + sum(j < i for j in halved) + part
        if i in halved:
            area = (span, pl.ds(part * half, half))
            return pltpu.make_async_copy(flat_values.at[area], vbuf.at[area], load_sem.at[at])
        return pltpu.make_async_copy(flat_values.at[span], vbuf.at[span], load_sem.at[at])

    barrier = pltpu.get_barrier_semaphore()
    pl.semaphore_signal(barrier, inc=1, device_id=(path_at, partner), device_id_type=MESH)

    @pl.when(leads)
    def _():
        for other in lead_peers:
            pl.semaphore_signal(barrier, inc=1, device_id=(path_at, other), device_id_type=MESH)

    copy_trades = pltpu.make_async_copy(trade_in, ts, small_sem.at[0])
    copy_hazard = pltpu.make_async_copy(hazard_in, hz, small_sem.at[1])
    copy_spread = pltpu.make_async_copy(spread_in, spread, small_sem.at[2])
    copy_trades.start()
    copy_hazard.start()
    copy_spread.start()
    for i in range(chunks):
        load(i, 0).start()
        if i in halved:
            load(i, 1).start()
    for z in range(1, n_path):
        @pl.when(z > path_at)
        def _():
            pl.semaphore_signal(barrier, inc=1, device_id=(z, me), device_id_type=MESH)

    def remote(src, dst, send, recv_at, device):
        return pltpu.make_async_remote_copy(
            src_ref=src, dst_ref=dst, send_sem=send, recv_sem=recv_at, device_id=device, device_id_type=MESH
        )

    def chunk_span(i):
        return pl.ds(pl.multiple_of(first[i] * CHUNK_PATHS, CHUNK_PATHS), CHUNK_PATHS)

    def own_rows(index):
        return pl.ds(pl.multiple_of(index * own, own), own)

    def row_copy(src, dst, arrival, other):
        return remote(src, dst, h_send, h_recv.at[arrival], (path_at, other))

    def hazards(count, arrival):
        span = hbuf.at[pl.ds(0, count)]
        return remote(span, span, h_send, h_recv.at[arrival], (path_at, partner))

    def from_chips(arrival, chips_there):
        for c in range(1, chips):
            @pl.when(chips_there == c)
            def _():
                hazards(c, arrival).wait_recv()

    def both_rows(q):
        return pl.ds(pl.multiple_of(q * 2 * own, 2 * own), 2 * own)

    def pair_copy(q, span):
        return remote(contrib.at[span], theirs.at[span], p_send, p_recv.at[q], (path_at, partner))

    def per_core(q, act):
        @pl.when(leads)
        def _():
            act(q, own_rows(q * 2), both_rows(q))

        @pl.when(jnp.logical_not(leads))
        def _():
            act(q, both_rows(q), own_rows(q * 2))

    def block_copy(q, slot_at):
        return remote(comb.at[own_rows(q * 2 + core)], recv.at[slot_at], b_send, b_recv, (path_at, q * 2 + core))

    def set_row(z, other):
        piece = lax.div((z * n_tm + other) * share, LANES)
        return remote(row_a.at[piece], rows_a.at[slot], a_send, a_recv, (z, other))

    def set_rows(count):
        span = rows_a.at[pl.ds(0, count)]
        return remote(span, span, a_send, a_recv, (path_at, partner))

    copy_trades.wait()
    base = lax.broadcasted_iota(jnp.int32, (PACK, LANES), 0)
    set_at = [(base + PACK * r).astype(f32).astype(bf16) for r in range(SETS // PACK)]
    one, zero = jnp.ones((PACK, LANES), bf16), jnp.zeros((PACK, LANES), bf16)
    for block in range(trades // LANES):
        ids = jnp.broadcast_to(ts[pl.ds(block, 1), :], (PACK, LANES)).astype(f32).astype(bf16)
        for r in range(SETS // PACK):
            picked = jnp.where(ids == set_at[r], one, zero)
            oh[pl.ds(r * PACK, PACK), pl.ds(block * LANES, LANES)] = picked.astype(oh.dtype)

    copy_hazard.wait()
    copy_spread.wait()
    total = jnp.zeros((1, paths), f32)
    weight_rows = []
    scale = 1.0 / (dates * n_tm)
    for d in range(dates):
        total = total + hz[pl.ds(d, 1), :]
        weight_rows.append((spread[d] * scale) * jnp.exp(-total))
    weight_rows.append(jnp.zeros((8 - dates, paths), f32))
    wt[...] = jnp.transpose(jnp.concatenate(weight_rows, axis=0))
    bsum[...] = total

    def meet():
        pl.semaphore_wait(barrier, 1 + path_at + core * (chips - 1))

        @pl.when(jnp.logical_not(leads))
        def _():
            row_copy(bsum, mate_sum, 0, partner).start()
            pl.semaphore_signal(mate, inc=1, device_id=(path_at, partner), device_id_type=MESH)

        @pl.when(leads)
        def _():
            pl.semaphore_wait(mate, 1)
            for other in lead_peers:
                pl.semaphore_signal(ready, inc=1, device_id=(path_at, other), device_id_type=MESH)
            row_copy(bsum, mate_sum, 0, partner).wait_recv()
            hbuf[chip] = bsum[...] + mate_sum[...]
            for k in range(1, chips):
                there = lax.rem(chip + k, chips)
                row_copy(hbuf.at[chip], hbuf.at[chip], jnp.where(there > chip, 1, 2), there * 2 + 1).start()

    def exchange(i):
        for k in range(per // 2):
            per_core(first[i] * (per // 2) + k, lambda q, send, take: pair_copy(q, send).start())

    def combine(q):
        per_core(q, lambda q, send, take: pair_copy(q, take).wait_recv())

        @pl.when(leads)
        def _():
            span = both_rows(q)
            both = theirs[span, :] + pcol[span, 0:1] * contrib[span, :]
            comb[span, :] = both
            upper = both.astype(bf16)
            limbs[0, span, :] = upper
            limbs[1, span, :] = (both - upper.astype(f32)).astype(bf16)

        @pl.when(jnp.logical_not(leads))
        def _():
            span = own_rows(q * 2)
            comb[span, :] = contrib[span, :] + pcol[span, 0:1] * theirs[span, :]

    own_chips = [my_chunk * (per // 2) + lax.rem(lax.rem(chip, per // 2) + k, per // 2) for k in range(per // 2)]
    other_chips = [first[i] * (per // 2) + k for i in range(chunks - 1) for k in range(per // 2)]
    other_chips += own_chips[1:]

    tiles = trades // TILE // 2

    def push(n):
        for unit in range(2):
            ids = oh[:, pl.ds((2 * (n % tiles) + unit) * TILE, TILE)]
            pltpu.matmul_push_rhs(ids, staging_register=n % 2, mxu_index=unit, transpose=True)

    def multiply(i, steps):
        span = pl.ds(pl.multiple_of(first[i] * rows, rows), rows)
        for t in steps:
            n = i * tiles + t
            if n + 1 < chunks * tiles:
                push(n + 1)
            for unit in range(2):
                block = vbuf[span, pl.ds((2 * t + unit) * TILE, TILE)]
                pltpu.matmul_acc_lhs(totals[unit * 2 + i % 2], block, load_staged_rhs=n % 2)

    def weigh(i):
        netted = pltpu.matmul_pop(totals[i % 2]) + pltpu.matmul_pop(totals[2 + i % 2])
        for h in range(SETS // LANES):
            nbuf[i, h] = netted[:, h * LANES : (h + 1) * LANES]
        path_span = chunk_span(i)
        weight = wt[path_span, :]
        for h in range(SETS // LANES):
            part = None
            for d in range(dates):
                picked = nbuf[i, h, pl.ds(d, CHUNK_PATHS, stride=dates), :]
                term = weight[:, d : d + 1] * jnp.maximum(picked, 0.0)
                part = term if part is None else part + term
            contrib[path_span, pl.ds(h * LANES, LANES)] = part

    @pl.when(jnp.logical_not(leads))
    def _():
        meet()

    push(0)
    for i in range(chunks):
        load(i, 0).wait()
        if i > 0:
            weigh(i - 1)
        multiply(i, range(tiles // 2 if i in halved else tiles))
        if i in halved:
            load(i, 1).wait()
            multiply(i, range(tiles // 2, tiles))
        if i == BARRIER_AFTER:
            @pl.when(leads)
            def _():
                meet()
        if i > 0 and i >= BARRIER_AFTER:
            for j in range(0 if i == max(BARRIER_AFTER, 1) else i - 1, i):
                exchange(j)
    weigh(chunks - 1)
    exchange(chunks - 1)

    @pl.when(jnp.logical_not(leads))
    def _():
        mate_sum[...] = bsum[...]
    pcol[...] = jnp.transpose(jnp.broadcast_to(jnp.exp(-mate_sum[...]), (8, paths)))
    @pl.when(leads)
    def _():
        pl.semaphore_wait(ready, chips - 1)
        pl.semaphore_signal(mate, inc=1, device_id=(path_at, partner), device_id_type=MESH)
        for z in range(n_path - 1):
            @pl.when(z < path_at)
            def _():
                pl.semaphore_signal(above, inc=1, device_id=(z, me), device_id_type=MESH)

    @pl.when(jnp.logical_not(leads))
    def _():
        combine(other_chips[0])
        pl.semaphore_wait(mate, 1)
        block_copy(other_chips[0], chip).start()

    @pl.when(leads)
    def _():
        combine(other_chips[0])

    for q in other_chips[1:]:
        combine(q)

        @pl.when(jnp.logical_not(leads))
        def _():
            block_copy(q, chip).start()

    combine(own_chips[0])

    def limb(unit, t, part):
        block = limbs[part, pl.ds((unit * row_tiles + t) * TILE, TILE), :]
        pltpu.matmul_push_rhs(block, staging_register=part, mxu_index=unit)

    row_tiles = paths // TILE // 2
    @pl.when(leads)
    def _():
        for unit in range(2):
            for part in range(2):
                limb(unit, 0, part)
        from_chips(1, chip)
        before_me[...] = jnp.zeros((1, paths), f32)
        for c in range(1, chips):
            @pl.when(chip == c)
            def _():
                before_me[...] = sum(hbuf[k] for k in range(c))
        earlier = jnp.broadcast_to(jnp.exp(-before_me[...]), (PACK, paths))
        upper = earlier.astype(bf16).astype(f32)
        at = lax.broadcasted_iota(jnp.int32, (PACK, paths), 0)
        weights = jnp.where(at == 0, upper, jnp.where(at == 1, earlier - upper, 0.0)).astype(bf16)
        for t in range(row_tiles):
            for unit in range(2):
                if t > 0:
                    limb(unit, t, 0)
                    limb(unit, t, 1)
                begin = (unit * row_tiles + t) * TILE
                for part in range(2):
                    pltpu.matmul_acc_lhs(totals[4 + unit], weights[:, begin : begin + TILE], load_staged_rhs=part)
        both = pltpu.matmul_pop(totals[4]) + pltpu.matmul_pop(totals[5])
        line = (both[0:1] + both[1:2]) * (1.0 / (paths * n_path))
        for h in range(SETS // LANES):
            row_a[h] = line[:, h * LANES : (h + 1) * LANES]
        for z in range(n_path - 1):
            @pl.when(z < path_at)
            def _():
                for k in range(n_tm):
                    set_row(z, lax.rem(me + 1 + k, n_tm)).start()
        for other in peers:
            set_row(path_at, other).start()

        for q in other_chips:
            block_copy(q, chip).start()
        from_chips(2, chips - 1 - chip)
        row_copy(hbuf, hbuf, 0, partner).start()
        @pl.when(path_at < n_path - 1)
        def _():
            pl.semaphore_wait(above, n_path - 1 - path_at)
        for z in range(1, n_path):
            @pl.when(z > path_at)
            def _():
                for k in range(n_tm):
                    set_row(z, lax.rem(me + 1 + k, n_tm)).start()
        rows_a[slot] = row_a[lax.div(flat * share, LANES)]

    @pl.when(jnp.logical_not(leads))
    def _():
        hazards(chips, 0).wait_recv()
    before = jnp.zeros((1, paths), f32)
    prefix = []
    for k in range(chips):
        prefix.append(before)
        before = before + hbuf[k]
    if chips < 8:
        prefix.append(jnp.zeros((8 - chips, paths), f32))
    ecol[...] = jnp.transpose(jnp.exp(-jnp.concatenate(prefix, axis=0)))
    factor = ecol[own_rows(me), :]
    recv[chip] = comb[own_rows(me), :]

    span = recv.at[pl.ds(0, chips - 1)]
    blocks = remote(span, span, b_send, b_recv, (path_at, partner))
    blocks.wait_recv()
    result = None
    for k in range(chips):
        term = factor[:, k : k + 1] * recv[k]
        result = term if result is None else result + term
    out[...] = result

    @pl.when(leads)
    def _():
        set_rows(senders - 1).wait_recv()

    @pl.when(jnp.logical_not(leads))
    def _():
        set_rows(senders).wait_recv()
    sums = jnp.broadcast_to(jnp.sum(rows_a[...], axis=0), (8, LANES))
    turned = pltpu.roll(sums, lax.rem(LANES - lax.rem(flat * share, LANES), LANES), 1)
    set_out[...] = turned[:1, :share]

    blocks.wait_send()

    @pl.when(leads)
    def _():
        hazards(chips, 0).wait_send()
        hazards(chips - 1, 0).wait_send()
        span = rows_a.at[pl.ds(0, senders - 1)]
        sent = remote(span, span, a_send, a_recv, (path_at, partner))
        sent.wait_send()
        span = rows_a.at[pl.ds(0, senders)]
        sent = remote(span, span, a_send, a_recv, (path_at, partner))
        sent.wait_send()
        span = theirs.at[pl.ds(0, paths // 2)]
        remote(span, span, p_send, p_recv.at[0], (path_at, partner)).wait_send()

    @pl.when(jnp.logical_not(leads))
    def _():
        row_copy(bsum, mate_sum, 0, partner).wait_send()
        remote(theirs, theirs, p_send, p_recv.at[0], (path_at, partner)).wait_send()


def finish(pathwise, sets, pathwise_out, sets_out, sem):
    copies = [
        pltpu.make_async_copy(pathwise, pathwise_out, sem.at[0]),
        pltpu.make_async_copy(sets, sets_out, sem.at[1]),
    ]
    for copy in copies:
        copy.start()
    for copy in copies:
        copy.wait()


def solution(mesh):
    n_path, n_tm = mesh.shape["path"], mesh.shape["tm"]
    n_all = n_path * n_tm

    def on_device(values, hazard, spread, trade_set):
        paths, dates, trades = values.shape
        own = paths // n_tm
        chunks = paths // CHUNK_PATHS
        f32 = jnp.float32
        hbm = pl.BlockSpec(memory_space=pltpu.HBM)
        vmem = pl.BlockSpec(memory_space=pltpu.VMEM)
        dma = pltpu.SemaphoreType.DMA
        pathwise, sets = pl.pallas_call(
            functools.partial(kernel, n_path, n_tm),
            out_shape=(pltpu.VMEM((own, SETS), f32), pltpu.VMEM((1, SETS // n_all), f32)),
            in_specs=[hbm, hbm, hbm, hbm],
            out_specs=(vmem, vmem),
            scratch_shapes=[
                pltpu.VMEM((paths * dates, trades), jnp.bfloat16),
                pltpu.VMEM((trades // LANES, LANES), jnp.int32),
                pltpu.VMEM((SETS, trades), jnp.float8_e4m3fn),
                pltpu.VMEM((dates, paths), f32),
                pltpu.SMEM((dates,), f32),
                pltpu.VMEM((chunks, SETS // LANES, CHUNK_PATHS * dates, LANES), f32),
                pltpu.VMEM((paths, 8), f32),
                pltpu.VMEM((paths, SETS), f32),
                pltpu.VMEM((paths, SETS), f32),
                pltpu.VMEM((paths, SETS), f32),
                pltpu.VMEM((n_tm // 2, own, SETS), f32),
                pltpu.VMEM((1, paths), f32),
                pltpu.VMEM((1, paths), f32),
                pltpu.VMEM((1, paths), f32),
                pltpu.VMEM((n_tm // 2, 1, paths), f32),
                pltpu.VMEM((paths, 8), f32),
                pltpu.VMEM((paths, max(8, n_tm // 2)), f32),
                pltpu.VMEM((2, paths, SETS), jnp.bfloat16),
                pltpu.VMEM((SETS // LANES, 1, LANES), f32),
                pltpu.VMEM((n_all // 2, 1, LANES), f32),
                dma((2 * chunks,)),
                dma((3,)),
                dma,
                dma((3,)),
                dma,
                dma((n_tm // 2,)),
                dma,
                dma,
                dma,
                dma,
                pltpu.SemaphoreType.REGULAR,
                pltpu.SemaphoreType.REGULAR,
                pltpu.SemaphoreType.REGULAR,
            ],
            compiler_params=pltpu.CompilerParams(
                collective_id=0, has_side_effects=True, vmem_limit_bytes=62 * 1024 * 1024
            ),
        )(values, hazard, spread, trade_set.reshape(trades // LANES, LANES))
        pathwise = pltpu.with_memory_space_constraint(pathwise, pltpu.VMEM)
        sets = pltpu.with_memory_space_constraint(sets, pltpu.VMEM)
        pathwise, sets = pl.pallas_call(
            finish,
            out_shape=(
                jax.ShapeDtypeStruct(pathwise.shape, f32),
                jax.ShapeDtypeStruct(sets.shape, f32),
            ),
            in_specs=[vmem, vmem],
            out_specs=(hbm, hbm),
            scratch_shapes=[dma((2,))],
        )(pathwise, sets)
        return pathwise, sets.reshape(SETS // n_all)

    in_specs = (P("path", "tm", None), P("tm", "path"), P("tm"), P())
    out_specs = (P(("path", "tm"), None), P(("path", "tm")))
    return jax.shard_map(
        on_device, mesh=mesh, in_specs=in_specs, out_specs=out_specs, check_vma=False
    )
```

```python
import functools

import jax
import jax.numpy as jnp
from jax import lax
from jax.experimental import pallas as pl
from jax.experimental.pallas import tpu as pltpu
from jax.sharding import PartitionSpec as P

SETS = 256
CHUNK_PATHS = 128
LANES = 128
PACK = 16
TILE = 256
BARRIER_AFTER = 1
MESH = pl.DeviceIdType.MESH


def kernel(n_path, n_tm, *refs):
    rows = CHUNK_PATHS * refs[0].shape[1]
    sums = [pltpu.ACC(unit)((rows, SETS), jnp.float32) for unit in (0, 0, 1, 1)]
    sums += [pltpu.ACC(unit)((PACK, SETS), jnp.float32) for unit in (0, 1)]
    sums += [pltpu.ACC(unit)((rows // 2, SETS), jnp.float32) for unit in (0, 0, 1, 1)]
    pl.run_scoped(lambda *totals: body(n_path, n_tm, totals, *refs), *sums)


def body(
    n_path, n_tm, totals, values, hazard_in, spread_in, trade_in, out, set_out,
    vbuf, ts, oh, hz, spread, nbuf, wt, contrib, theirs, comb, recv, bsum, mate_sum, before_me, erow, hbuf, pcol, ecol, limbs, row_a, rows_a,
    load_sem, small_sem, h_recv, p_recv, b_recv, a_recv, mate, ready, above,
):
    paths, dates, trades = values.shape
    f32, bf16 = jnp.float32, jnp.bfloat16
    own = paths // n_tm
    chunks = paths // CHUNK_PATHS
    per = n_tm // chunks
    n_all = n_path * n_tm
    chips = n_tm // 2
    share = SETS // n_all
    path_at, me = lax.axis_index("path"), lax.axis_index("tm")
    flat = path_at * n_tm + me
    chip, core = lax.div(me, 2), lax.rem(me, 2)
    partner = me + 1 - 2 * core
    peers = [lax.rem(me + k, n_tm) for k in range(1, n_tm)]
    leads = core == 1
    lead_peers = [lax.rem(chip + k, chips) * 2 + 1 for k in range(1, chips)]
    senders = n_path * chips
    slot = path_at * chips + chip
    rows = CHUNK_PATHS * dates
    my_chunk = lax.div(me, per)
    if chunks == 4:
        high, low = lax.div(my_chunk, 2), lax.rem(my_chunk, 2)
        first = [2 * (1 - high) + 1 - low, 2 * high + 1 - low, 2 * (1 - high) + low, my_chunk]
    else:
        first = [lax.rem(my_chunk + 1 + i, chunks) for i in range(chunks)]
    flat_values = values.reshape(paths * dates, trades)

    last = chunks - 1
    h_send, p_send, b_send, a_send = small_sem.at[0], load_sem.at[0], load_sem.at[1], load_sem.at[2]

    def load(i, part):
        begin = pl.multiple_of(first[i] * rows, rows)
        if i == last:
            area = (pl.ds(pl.multiple_of(begin + part * rows // 2, rows // 2), rows // 2), slice(None))
        else:
            area = (pl.ds(begin, rows), pl.ds(part * trades // 2, trades // 2))
        return pltpu.make_async_copy(flat_values.at[area], vbuf.at[area], load_sem.at[2 * i + part])

    barrier = pltpu.get_barrier_semaphore()
    pl.semaphore_signal(barrier, inc=1, device_id=(path_at, partner), device_id_type=MESH)

    @pl.when(leads)
    def _():
        for other in lead_peers:
            pl.semaphore_signal(barrier, inc=1, device_id=(path_at, other), device_id_type=MESH)

    copy_hazard = pltpu.make_async_copy(hazard_in, hz, small_sem.at[0])
    copy_trades = pltpu.make_async_copy(trade_in, ts, small_sem.at[1])
    copy_spread = pltpu.make_async_copy(spread_in, spread, small_sem.at[2])
    copy_hazard.start()
    copy_trades.start()
    copy_spread.start()
    for i in range(chunks):
        for part in range(2):
            load(i, part).start()
    for z in range(1, n_path):
        @pl.when(z > path_at)
        def _():
            pl.semaphore_signal(barrier, inc=1, device_id=(z, me), device_id_type=MESH)

    def remote(src, dst, send, recv_at, device):
        return pltpu.make_async_remote_copy(
            src_ref=src, dst_ref=dst, send_sem=send, recv_sem=recv_at, device_id=device, device_id_type=MESH
        )

    def chunk_span(i):
        return pl.ds(pl.multiple_of(first[i] * CHUNK_PATHS, CHUNK_PATHS), CHUNK_PATHS)

    def own_rows(index):
        return pl.ds(pl.multiple_of(index * own, own), own)

    def row_copy(src, dst, arrival, other):
        return remote(src, dst, h_send, h_recv.at[arrival], (path_at, other))

    def hazards(count, arrival):
        span = hbuf.at[pl.ds(0, count)]
        return remote(span, span, h_send, h_recv.at[arrival], (path_at, partner))

    def from_chips(arrival, chips_there):
        for c in range(1, chips):
            @pl.when(chips_there == c)
            def _():
                hazards(c, arrival).wait_recv()

    def both_rows(q):
        return pl.ds(pl.multiple_of(q * 2 * own, 2 * own), 2 * own)

    def pair_copy(q, span):
        return remote(contrib.at[span], theirs.at[span], p_send, p_recv.at[q], (path_at, partner))

    def per_core(q, act):
        @pl.when(leads)
        def _():
            act(q, own_rows(q * 2), both_rows(q))

        @pl.when(jnp.logical_not(leads))
        def _():
            act(q, both_rows(q), own_rows(q * 2))

    def block_copy(q, slot_at):
        return remote(comb.at[own_rows(q * 2 + core)], recv.at[slot_at], b_send, b_recv, (path_at, q * 2 + core))

    def set_row(z, other):
        piece = lax.div((z * n_tm + other) * share, LANES)
        return remote(row_a.at[piece], rows_a.at[slot], a_send, a_recv, (z, other))

    def set_rows(count):
        span = rows_a.at[pl.ds(0, count)]
        return remote(span, span, a_send, a_recv, (path_at, partner))

    copy_hazard.wait()
    bsum[...] = sum(hz[pl.ds(d, 1), :] for d in range(dates))

    def meet():
        pl.semaphore_wait(barrier, 1 + path_at + core * (chips - 1))

        @pl.when(jnp.logical_not(leads))
        def _():
            row_copy(bsum, mate_sum, 0, partner).start()
            pl.semaphore_signal(mate, inc=1, device_id=(path_at, partner), device_id_type=MESH)

        @pl.when(leads)
        def _():
            pl.semaphore_wait(mate, 1)
            for other in lead_peers:
                pl.semaphore_signal(ready, inc=1, device_id=(path_at, other), device_id_type=MESH)
            row_copy(bsum, mate_sum, 0, partner).wait_recv()
            hbuf[chip] = bsum[...] + mate_sum[...]
            for k in range(1, chips):
                there = lax.rem(chip + k, chips)
                row_copy(hbuf.at[chip], hbuf.at[chip], jnp.where(there > chip, 1, 2), there * 2 + 1).start()

    @pl.when(jnp.logical_not(leads))
    def _():
        meet()
    copy_trades.wait()
    base = lax.broadcasted_iota(jnp.int32, (PACK, LANES), 0)
    set_at = [(base + PACK * r).astype(f32).astype(bf16) for r in range(SETS // PACK)]
    one, zero = jnp.ones((PACK, LANES), bf16), jnp.zeros((PACK, LANES), bf16)
    for block in range(trades // LANES):
        ids = jnp.broadcast_to(ts[pl.ds(block, 1), :], (PACK, LANES)).astype(f32).astype(bf16)
        for r in range(SETS // PACK):
            picked = jnp.where(ids == set_at[r], one, zero)
            oh[pl.ds(r * PACK, PACK), pl.ds(block * LANES, LANES)] = picked.astype(oh.dtype)

    copy_spread.wait()
    total = jnp.zeros((1, paths), f32)
    weight_rows = []
    scale = 1.0 / (dates * n_tm)
    for d in range(dates):
        total = total + hz[pl.ds(d, 1), :]
        weight_rows.append((spread[d] * scale) * jnp.exp(-total))
    weight_rows.append(jnp.zeros((8 - dates, paths), f32))
    wt[...] = jnp.transpose(jnp.concatenate(weight_rows, axis=0))

    def exchange(i):
        for k in range(per // 2):
            per_core(first[i] * (per // 2) + k, lambda q, send, take: pair_copy(q, send).start())

    def exchange_half(part):
        chips_here = per // 2
        if chips_here > 1:
            for k in range(part * chips_here // 2, (part + 1) * chips_here // 2):
                per_core(first[last] * chips_here + k, lambda q, send, take: pair_copy(q, send).start())
            return

        @pl.when(jnp.logical_not(leads))
        def _():
            pair_copy(my_chunk, own_rows(my_chunk * 2 + part)).start()

        if part == 0:
            @pl.when(leads)
            def _():
                pair_copy(my_chunk, own_rows(my_chunk * 2)).start()

    def combine(q):
        per_core(q, lambda q, send, take: pair_copy(q, take).wait_recv())

        @pl.when(leads)
        def _():
            span = both_rows(q)
            both = theirs[span, :] + pcol[span, 0:1] * contrib[span, :]
            comb[span, :] = both
            upper = both.astype(bf16)
            limbs[0, span, :] = upper
            limbs[1, span, :] = (both - upper.astype(f32)).astype(bf16)

        @pl.when(jnp.logical_not(leads))
        def _():
            span = own_rows(q * 2)
            comb[span, :] = contrib[span, :] + pcol[span, 0:1] * theirs[span, :]

    own_chips = [my_chunk * (per // 2) + lax.rem(lax.rem(chip, per // 2) + k, per // 2) for k in range(per // 2)]
    other_chips = [first[i] * (per // 2) + k for i in range(chunks - 1) for k in range(per // 2)]
    other_chips += own_chips[1:]

    tiles = trades // TILE // 2

    def push(n):
        for unit in range(2):
            ids = oh[:, pl.ds((2 * (n % tiles) + unit) * TILE, TILE)]
            pltpu.matmul_push_rhs(ids, staging_register=n % 2, mxu_index=unit, transpose=True)

    def multiply(n, span, into, steps):
        for t in steps:
            if n + t + 1 < (chunks + 1) * tiles:
                push(n + t + 1)
            for unit in range(2):
                block = vbuf[span, pl.ds((2 * t + unit) * TILE, TILE)]
                pltpu.matmul_acc_lhs(into[unit], block, load_staged_rhs=(n + t) % 2)

    def weigh(i, begin, paths_here, done):
        netted = pltpu.matmul_pop(done[0]) + pltpu.matmul_pop(done[1])
        for h in range(SETS // LANES):
            nbuf[i, h, pl.ds(begin * dates, paths_here * dates)] = netted[:, h * LANES : (h + 1) * LANES]
        path_span = pl.ds(pl.multiple_of(first[i] * CHUNK_PATHS + begin, paths_here), paths_here)
        weight = wt[path_span, :]
        for h in range(SETS // LANES):
            part = None
            for d in range(dates):
                picked = nbuf[i, h, pl.ds(begin * dates + d, paths_here, stride=dates), :]
                term = weight[:, d : d + 1] * jnp.maximum(picked, 0.0)
                part = term if part is None else part + term
            contrib[path_span, pl.ds(h * LANES, LANES)] = part

    def whole(i):
        return totals[i % 2], totals[2 + i % 2]

    def in_half(part):
        return totals[6 + part], totals[8 + part]

    some = CHUNK_PATHS // 2
    push(0)
    for i in range(chunks):
        for part in range(2):
            load(i, part).wait()
            if part == 0 and i > 0:
                weigh(i - 1, 0, CHUNK_PATHS, whole(i - 1))
            if i < last:
                span = pl.ds(pl.multiple_of(first[i] * rows, rows), rows)
                steps = range(part * tiles // 2, (part + 1) * tiles // 2)
                multiply(i * tiles, span, whole(i), steps)
            else:
                if part == 1:
                    weigh(i, 0, some, in_half(0))
                begin = pl.multiple_of(first[i] * rows + part * rows // 2, rows // 2)
                multiply((i + part) * tiles, pl.ds(begin, rows // 2), in_half(part), range(tiles))
            if i == BARRIER_AFTER and part == 1:
                @pl.when(leads)
                def _():
                    meet()
            if i == last:
                if part == 0:
                    exchange(last - 1)
                else:
                    exchange_half(0)
            elif part == 1 and i > 0 and i >= BARRIER_AFTER:
                for j in range(0 if i == max(BARRIER_AFTER, 1) else i - 1, i):
                    exchange(j)
    weigh(last, some, some, in_half(1))
    exchange_half(1)

    @pl.when(jnp.logical_not(leads))
    def _():
        mate_sum[...] = bsum[...]
    pcol[...] = jnp.transpose(jnp.broadcast_to(jnp.exp(-mate_sum[...]), (8, paths)))
    @pl.when(leads)
    def _():
        pl.semaphore_wait(ready, chips - 1)
        pl.semaphore_signal(mate, inc=1, device_id=(path_at, partner), device_id_type=MESH)
        for z in range(n_path - 1):
            @pl.when(z < path_at)
            def _():
                pl.semaphore_signal(above, inc=1, device_id=(z, me), device_id_type=MESH)

    @pl.when(jnp.logical_not(leads))
    def _():
        combine(other_chips[0])
        pl.semaphore_wait(mate, 1)
        block_copy(other_chips[0], chip).start()

    @pl.when(leads)
    def _():
        combine(other_chips[0])

    for q in other_chips[1:]:
        combine(q)

        @pl.when(jnp.logical_not(leads))
        def _():
            block_copy(q, chip).start()

    @pl.when(leads)
    def _():
        from_chips(1, chip)
        before_me[...] = jnp.zeros((1, paths), f32)
        for c in range(1, chips):
            @pl.when(chip == c)
            def _():
                before_me[...] = sum(hbuf[k] for k in range(c))
        earlier = jnp.broadcast_to(jnp.exp(-before_me[...]), (PACK, paths))
        upper = earlier.astype(bf16).astype(f32)
        at = lax.broadcasted_iota(jnp.int32, (PACK, paths), 0)
        erow[...] = jnp.where(at == 0, upper, jnp.where(at == 1, earlier - upper, 0.0)).astype(bf16)

    combine(own_chips[0])

    def limb(unit, t, part):
        block = limbs[part, pl.ds((unit * row_tiles + t) * TILE, TILE), :]
        pltpu.matmul_push_rhs(block, staging_register=part, mxu_index=unit)

    row_tiles = paths // TILE // 2
    @pl.when(leads)
    def _():
        for unit in range(2):
            for part in range(2):
                limb(unit, 0, part)
        for t in range(row_tiles):
            for unit in range(2):
                if t > 0:
                    limb(unit, t, 0)
                    limb(unit, t, 1)
                begin = (unit * row_tiles + t) * TILE
                for part in range(2):
                    pltpu.matmul_acc_lhs(totals[4 + unit], erow[:, pl.ds(begin, TILE)], load_staged_rhs=part)
        both = pltpu.matmul_pop(totals[4]) + pltpu.matmul_pop(totals[5])
        line = (both[0:1] + both[1:2]) * (1.0 / (paths * n_path))
        for h in range(SETS // LANES):
            row_a[h] = line[:, h * LANES : (h + 1) * LANES]
        for z in range(n_path - 1):
            @pl.when(z < path_at)
            def _():
                for k in range(n_tm):
                    set_row(z, lax.rem(me + 1 + k, n_tm)).start()
        for other in peers:
            set_row(path_at, other).start()

        for q in other_chips:
            block_copy(q, chip).start()
        from_chips(2, chips - 1 - chip)
        row_copy(hbuf, hbuf, 0, partner).start()
        @pl.when(path_at < n_path - 1)
        def _():
            pl.semaphore_wait(above, n_path - 1 - path_at)
        for z in range(1, n_path):
            @pl.when(z > path_at)
            def _():
                for k in range(n_tm):
                    set_row(z, lax.rem(me + 1 + k, n_tm)).start()
        rows_a[slot] = row_a[lax.div(flat * share, LANES)]

    @pl.when(jnp.logical_not(leads))
    def _():
        hazards(chips, 0).wait_recv()
    before = jnp.zeros((1, paths), f32)
    prefix = []
    for k in range(chips):
        prefix.append(before)
        before = before + hbuf[k]
    if chips < 8:
        prefix.append(jnp.zeros((8 - chips, paths), f32))
    ecol[...] = jnp.transpose(jnp.exp(-jnp.concatenate(prefix, axis=0)))
    factor = ecol[own_rows(me), :]
    recv[chip] = comb[own_rows(me), :]

    span = recv.at[pl.ds(0, chips - 1)]
    blocks = remote(span, span, b_send, b_recv, (path_at, partner))
    blocks.wait_recv()
    result = None
    for k in range(chips):
        term = factor[:, k : k + 1] * recv[k]
        result = term if result is None else result + term
    out[...] = result

    @pl.when(leads)
    def _():
        set_rows(senders - 1).wait_recv()

    @pl.when(jnp.logical_not(leads))
    def _():
        set_rows(senders).wait_recv()
    sums = jnp.broadcast_to(jnp.sum(rows_a[...], axis=0), (8, LANES))
    turned = pltpu.roll(sums, lax.rem(LANES - lax.rem(flat * share, LANES), LANES), 1)
    set_out[...] = turned[:1, :share]

    blocks.wait_send()

    @pl.when(leads)
    def _():
        hazards(chips, 0).wait_send()
        hazards(chips - 1, 0).wait_send()
        span = rows_a.at[pl.ds(0, senders - 1)]
        sent = remote(span, span, a_send, a_recv, (path_at, partner))
        sent.wait_send()
        span = rows_a.at[pl.ds(0, senders)]
        sent = remote(span, span, a_send, a_recv, (path_at, partner))
        sent.wait_send()
        span = theirs.at[pl.ds(0, paths // 2)]
        remote(span, span, p_send, p_recv.at[0], (path_at, partner)).wait_send()

    @pl.when(jnp.logical_not(leads))
    def _():
        row_copy(bsum, mate_sum, 0, partner).wait_send()
        remote(theirs, theirs, p_send, p_recv.at[0], (path_at, partner)).wait_send()


def finish(pathwise, sets, pathwise_out, sets_out, sem):
    copies = [
        pltpu.make_async_copy(pathwise, pathwise_out, sem.at[0]),
        pltpu.make_async_copy(sets, sets_out, sem.at[1]),
    ]
    for copy in copies:
        copy.start()
    for copy in copies:
        copy.wait()


def solution(mesh):
    n_path, n_tm = mesh.shape["path"], mesh.shape["tm"]
    n_all = n_path * n_tm

    def on_device(values, hazard, spread, trade_set):
        paths, dates, trades = values.shape
        own = paths // n_tm
        chunks = paths // CHUNK_PATHS
        f32 = jnp.float32
        hbm = pl.BlockSpec(memory_space=pltpu.HBM)
        vmem = pl.BlockSpec(memory_space=pltpu.VMEM)
        dma = pltpu.SemaphoreType.DMA
        pathwise, sets = pl.pallas_call(
            functools.partial(kernel, n_path, n_tm),
            out_shape=(pltpu.VMEM((own, SETS), f32), pltpu.VMEM((1, SETS // n_all), f32)),
            in_specs=[hbm, hbm, hbm, hbm],
            out_specs=(vmem, vmem),
            scratch_shapes=[
                pltpu.VMEM((paths * dates, trades), jnp.bfloat16),
                pltpu.VMEM((trades // LANES, LANES), jnp.int32),
                pltpu.VMEM((SETS, trades), jnp.float8_e4m3fn),
                pltpu.VMEM((dates, paths), f32),
                pltpu.SMEM((dates,), f32),
                pltpu.VMEM((chunks, SETS // LANES, CHUNK_PATHS * dates, LANES), f32),
                pltpu.VMEM((paths, 8), f32),
                pltpu.VMEM((paths, SETS), f32),
                pltpu.VMEM((paths, SETS), f32),
                pltpu.VMEM((paths, SETS), f32),
                pltpu.VMEM((n_tm // 2, own, SETS), f32),
                pltpu.VMEM((1, paths), f32),
                pltpu.VMEM((1, paths), f32),
                pltpu.VMEM((1, paths), f32),
                pltpu.VMEM((PACK, paths), jnp.bfloat16),
                pltpu.VMEM((n_tm // 2, 1, paths), f32),
                pltpu.VMEM((paths, 8), f32),
                pltpu.VMEM((paths, max(8, n_tm // 2)), f32),
                pltpu.VMEM((2, paths, SETS), jnp.bfloat16),
                pltpu.VMEM((SETS // LANES, 1, LANES), f32),
                pltpu.VMEM((n_all // 2, 1, LANES), f32),
                dma((2 * chunks,)),
                dma((3,)),
                dma((3,)),
                dma((n_tm // 2,)),
                dma,
                dma,
                pltpu.SemaphoreType.REGULAR,
                pltpu.SemaphoreType.REGULAR,
                pltpu.SemaphoreType.REGULAR,
            ],
            compiler_params=pltpu.CompilerParams(
                collective_id=0, has_side_effects=True, vmem_limit_bytes=62 * 1024 * 1024
            ),
        )(values, hazard, spread, trade_set.reshape(trades // LANES, LANES))
        pathwise = pltpu.with_memory_space_constraint(pathwise, pltpu.VMEM)
        sets = pltpu.with_memory_space_constraint(sets, pltpu.VMEM)
        pathwise, sets = pl.pallas_call(
            finish,
            out_shape=(
                jax.ShapeDtypeStruct(pathwise.shape, f32),
                jax.ShapeDtypeStruct(sets.shape, f32),
            ),
            in_specs=[vmem, vmem],
            out_specs=(hbm, hbm),
            scratch_shapes=[dma((2,))],
        )(pathwise, sets)
        return pathwise, sets.reshape(SETS // n_all)

    in_specs = (P("path", "tm", None), P("tm", "path"), P("tm"), P())
    out_specs = (P(("path", "tm"), None), P(("path", "tm")))
    return jax.shard_map(
        on_device, mesh=mesh, in_specs=in_specs, out_specs=out_specs, check_vma=False
    )
```

```python
import functools

import jax
import jax.numpy as jnp
from jax import lax
from jax.experimental import pallas as pl
from jax.experimental.pallas import tpu as pltpu
from jax.sharding import PartitionSpec as P

SETS = 256
CHUNK_PATHS = 128
LANES = 128
PACK = 16
TILE = 256
BARRIER_AFTER = 1
MESH = pl.DeviceIdType.MESH


def kernel(n_path, n_tm, *refs):
    rows = CHUNK_PATHS * refs[0].shape[1]
    sums = [pltpu.ACC(unit)((rows, SETS), jnp.float32) for unit in (0, 0, 1, 1)]
    sums += [pltpu.ACC(unit)((PACK, SETS), jnp.float32) for unit in (0, 1)]
    sums += [pltpu.ACC(unit)((rows // 2, SETS), jnp.float32) for unit in (0, 0, 1, 1)]
    pl.run_scoped(lambda *totals: body(n_path, n_tm, totals, *refs), *sums)


def body(
    n_path, n_tm, totals, values, hazard_in, spread_in, trade_in, out, set_out,
    vbuf, ts, oh, hz, spread, nbuf, wt, contrib, theirs, comb, recv, bsum, mate_sum, before_me, erow, hbuf, pcol, ecol, limbs, row_a, rows_a,
    load_sem, small_sem, h_recv, p_recv, b_recv, a_recv, mate, ready, above,
):
    paths, dates, trades = values.shape
    f32, bf16 = jnp.float32, jnp.bfloat16
    own = paths // n_tm
    chunks = paths // CHUNK_PATHS
    per = n_tm // chunks
    n_all = n_path * n_tm
    chips = n_tm // 2
    share = SETS // n_all
    path_at, me = lax.axis_index("path"), lax.axis_index("tm")
    flat = path_at * n_tm + me
    chip, core = lax.div(me, 2), lax.rem(me, 2)
    partner = me + 1 - 2 * core
    peers = [lax.rem(me + k, n_tm) for k in range(1, n_tm)]
    leads = core == 1
    lead_peers = [lax.rem(chip + k, chips) * 2 + 1 for k in range(1, chips)]
    senders = n_path * chips
    slot = path_at * chips + chip
    rows = CHUNK_PATHS * dates
    my_chunk = lax.div(me, per)
    if chunks == 4:
        high, low = lax.div(my_chunk, 2), lax.rem(my_chunk, 2)
        first = [2 * (1 - high) + 1 - low, 2 * high + 1 - low, 2 * (1 - high) + low, my_chunk]
    else:
        first = [lax.rem(my_chunk + 1 + i, chunks) for i in range(chunks)]
    flat_values = values.reshape(paths * dates, trades)

    last = chunks - 1
    h_send, p_send, b_send, a_send = small_sem.at[0], load_sem.at[0], load_sem.at[1], load_sem.at[2]

    def load(i, part):
        begin = pl.multiple_of(first[i] * rows, rows)
        if i == last:
            area = (pl.ds(pl.multiple_of(begin + part * rows // 2, rows // 2), rows // 2), slice(None))
        else:
            area = (pl.ds(begin, rows), pl.ds(part * trades // 2, trades // 2))
        return pltpu.make_async_copy(flat_values.at[area], vbuf.at[area], load_sem.at[2 * i + part])

    barrier = pltpu.get_barrier_semaphore()
    pl.semaphore_signal(barrier, inc=1, device_id=(path_at, partner), device_id_type=MESH)

    @pl.when(leads)
    def _():
        for other in lead_peers:
            pl.semaphore_signal(barrier, inc=1, device_id=(path_at, other), device_id_type=MESH)

    copy_hazard = pltpu.make_async_copy(hazard_in, hz, small_sem.at[0])
    copy_trades = pltpu.make_async_copy(trade_in, ts, small_sem.at[1])
    copy_spread = pltpu.make_async_copy(spread_in, spread, small_sem.at[2])
    copy_hazard.start()
    copy_trades.start()
    copy_spread.start()
    for i in range(chunks):
        for part in range(2):
            load(i, part).start()
    for z in range(1, n_path):
        @pl.when(z > path_at)
        def _():
            pl.semaphore_signal(barrier, inc=1, device_id=(z, me), device_id_type=MESH)

    def remote(src, dst, send, recv_at, device):
        return pltpu.make_async_remote_copy(
            src_ref=src, dst_ref=dst, send_sem=send, recv_sem=recv_at, device_id=device, device_id_type=MESH
        )

    def chunk_span(i):
        return pl.ds(pl.multiple_of(first[i] * CHUNK_PATHS, CHUNK_PATHS), CHUNK_PATHS)

    def own_rows(index):
        return pl.ds(pl.multiple_of(index * own, own), own)

    def row_copy(src, dst, arrival, other):
        return remote(src, dst, h_send, h_recv.at[arrival], (path_at, other))

    def hazards(count, arrival):
        span = hbuf.at[pl.ds(0, count)]
        return remote(span, span, h_send, h_recv.at[arrival], (path_at, partner))

    def from_chips(arrival, chips_there):
        for c in range(1, chips):
            @pl.when(chips_there == c)
            def _():
                hazards(c, arrival).wait_recv()

    def both_rows(q):
        return pl.ds(pl.multiple_of(q * 2 * own, 2 * own), 2 * own)

    def pair_copy(q, span):
        return remote(contrib.at[span], theirs.at[span], p_send, p_recv.at[q], (path_at, partner))

    def per_core(q, act):
        @pl.when(leads)
        def _():
            act(q, own_rows(q * 2), both_rows(q))

        @pl.when(jnp.logical_not(leads))
        def _():
            act(q, both_rows(q), own_rows(q * 2))

    def block_copy(q, slot_at):
        return remote(comb.at[own_rows(q * 2 + core)], recv.at[slot_at], b_send, b_recv, (path_at, q * 2 + core))

    def set_row(z, other):
        piece = lax.div((z * n_tm + other) * share, LANES)
        return remote(row_a.at[piece], rows_a.at[slot], a_send, a_recv, (z, other))

    def set_rows(count):
        span = rows_a.at[pl.ds(0, count)]
        return remote(span, span, a_send, a_recv, (path_at, partner))

    copy_hazard.wait()
    bsum[...] = sum(hz[pl.ds(d, 1), :] for d in range(dates))

    def meet():
        pl.semaphore_wait(barrier, 1 + path_at + core * (chips - 1))

        @pl.when(jnp.logical_not(leads))
        def _():
            row_copy(bsum, mate_sum, 0, partner).start()
            pl.semaphore_signal(mate, inc=1, device_id=(path_at, partner), device_id_type=MESH)

        @pl.when(leads)
        def _():
            pl.semaphore_wait(mate, 1)
            for other in lead_peers:
                pl.semaphore_signal(ready, inc=1, device_id=(path_at, other), device_id_type=MESH)
            row_copy(bsum, mate_sum, 0, partner).wait_recv()
            hbuf[chip] = bsum[...] + mate_sum[...]
            for k in range(1, chips):
                there = lax.rem(chip + k, chips)
                row_copy(hbuf.at[chip], hbuf.at[chip], jnp.where(there > chip, 1, 2), there * 2 + 1).start()

    @pl.when(jnp.logical_not(leads))
    def _():
        meet()
    copy_trades.wait()
    base = lax.broadcasted_iota(jnp.int32, (PACK, LANES), 0)
    set_at = [(base + PACK * r).astype(f32).astype(bf16) for r in range(SETS // PACK)]
    one, zero = jnp.ones((PACK, LANES), bf16), jnp.zeros((PACK, LANES), bf16)
    for block in range(trades // LANES):
        ids = jnp.broadcast_to(ts[pl.ds(block, 1), :], (PACK, LANES)).astype(f32).astype(bf16)
        for r in range(SETS // PACK):
            picked = jnp.where(ids == set_at[r], one, zero)
            oh[pl.ds(r * PACK, PACK), pl.ds(block * LANES, LANES)] = picked.astype(oh.dtype)

    copy_spread.wait()
    total = jnp.zeros((1, paths), f32)
    weight_rows = []
    scale = 1.0 / (dates * n_tm)
    for d in range(dates):
        total = total + hz[pl.ds(d, 1), :]
        weight_rows.append((spread[d] * scale) * jnp.exp(-total))
    weight_rows.append(jnp.zeros((8 - dates, paths), f32))
    wt[...] = jnp.transpose(jnp.concatenate(weight_rows, axis=0))

    def exchange(i):
        for k in range(per // 2):
            per_core(first[i] * (per // 2) + k, lambda q, send, take: pair_copy(q, send).start())

    def exchange_half(part):
        chips_here = per // 2
        if chips_here > 1:
            for k in range(part * chips_here // 2, (part + 1) * chips_here // 2):
                per_core(first[last] * chips_here + k, lambda q, send, take: pair_copy(q, send).start())
            return

        @pl.when(jnp.logical_not(leads))
        def _():
            pair_copy(my_chunk, own_rows(my_chunk * 2 + part)).start()

        if part == 0:
            @pl.when(leads)
            def _():
                pair_copy(my_chunk, own_rows(my_chunk * 2)).start()

    def combine(q):
        per_core(q, lambda q, send, take: pair_copy(q, take).wait_recv())

        @pl.when(leads)
        def _():
            span = both_rows(q)
            both = theirs[span, :] + pcol[span, 0:1] * contrib[span, :]
            comb[span, :] = both
            upper = both.astype(bf16)
            limbs[0, span, :] = upper
            limbs[1, span, :] = (both - upper.astype(f32)).astype(bf16)

        @pl.when(jnp.logical_not(leads))
        def _():
            span = own_rows(q * 2)
            comb[span, :] = contrib[span, :] + pcol[span, 0:1] * theirs[span, :]

    own_chips = [my_chunk * (per // 2) + lax.rem(lax.rem(chip, per // 2) + k, per // 2) for k in range(per // 2)]
    other_chips = [first[i] * (per // 2) + k for i in range(chunks - 1) for k in range(per // 2)]
    other_chips += own_chips[1:]

    tiles = trades // TILE // 2

    def push(n):
        for unit in range(2):
            ids = oh[:, pl.ds((2 * (n % tiles) + unit) * TILE, TILE)]
            pltpu.matmul_push_rhs(ids, staging_register=n % 2, mxu_index=unit, transpose=True)

    def multiply(n, span, into, steps):
        for t in steps:
            if n + t + 1 < (chunks + 1) * tiles:
                push(n + t + 1)
            for unit in range(2):
                block = vbuf[span, pl.ds((2 * t + unit) * TILE, TILE)]
                pltpu.matmul_acc_lhs(into[unit], block, load_staged_rhs=(n + t) % 2)

    def weigh(i, begin, paths_here, done):
        netted = pltpu.matmul_pop(done[0]) + pltpu.matmul_pop(done[1])
        for h in range(SETS // LANES):
            nbuf[i, h, pl.ds(begin * dates, paths_here * dates)] = netted[:, h * LANES : (h + 1) * LANES]
        path_span = pl.ds(pl.multiple_of(first[i] * CHUNK_PATHS + begin, paths_here), paths_here)
        weight = wt[path_span, :]
        for h in range(SETS // LANES):
            part = None
            for d in range(dates):
                picked = nbuf[i, h, pl.ds(begin * dates + d, paths_here, stride=dates), :]
                term = weight[:, d : d + 1] * jnp.maximum(picked, 0.0)
                part = term if part is None else part + term
            contrib[path_span, pl.ds(h * LANES, LANES)] = part

    def whole(i):
        return totals[i % 2], totals[2 + i % 2]

    def in_half(part):
        return totals[6 + part], totals[8 + part]

    some = CHUNK_PATHS // 2
    push(0)
    for i in range(chunks):
        for part in range(2):
            load(i, part).wait()
            if part == 0 and i > 0:
                weigh(i - 1, 0, CHUNK_PATHS, whole(i - 1))
            if i < last:
                span = pl.ds(pl.multiple_of(first[i] * rows, rows), rows)
                steps = range(part * tiles // 2, (part + 1) * tiles // 2)
                multiply(i * tiles, span, whole(i), steps)
            else:
                if part == 1:
                    weigh(i, 0, some, in_half(0))
                begin = pl.multiple_of(first[i] * rows + part * rows // 2, rows // 2)
                multiply((i + part) * tiles, pl.ds(begin, rows // 2), in_half(part), range(tiles))
            if i == BARRIER_AFTER and part == 1:
                @pl.when(leads)
                def _():
                    meet()
            if i == last:
                if part == 0:
                    exchange(last - 1)
                else:
                    exchange_half(0)
            elif part == 1 and i > 0 and i >= BARRIER_AFTER:
                for j in range(0 if i == max(BARRIER_AFTER, 1) else i - 1, i):
                    exchange(j)
    weigh(last, some, some, in_half(1))
    exchange_half(1)

    @pl.when(jnp.logical_not(leads))
    def _():
        mate_sum[...] = bsum[...]
    pcol[...] = jnp.transpose(jnp.broadcast_to(jnp.exp(-mate_sum[...]), (8, paths)))
    @pl.when(leads)
    def _():
        pl.semaphore_wait(ready, chips - 1)
        pl.semaphore_signal(mate, inc=1, device_id=(path_at, partner), device_id_type=MESH)
        for z in range(n_path - 1):
            @pl.when(z < path_at)
            def _():
                pl.semaphore_signal(above, inc=1, device_id=(z, me), device_id_type=MESH)

    @pl.when(jnp.logical_not(leads))
    def _():
        combine(other_chips[0])
        pl.semaphore_wait(mate, 1)
        block_copy(other_chips[0], chip).start()

    @pl.when(leads)
    def _():
        combine(other_chips[0])

    for q in other_chips[1:]:
        combine(q)

        @pl.when(jnp.logical_not(leads))
        def _():
            block_copy(q, chip).start()

    @pl.when(leads)
    def _():
        from_chips(1, chip)
        before_me[...] = jnp.zeros((1, paths), f32)
        for c in range(1, chips):
            @pl.when(chip == c)
            def _():
                before_me[...] = sum(hbuf[k] for k in range(c))
        earlier = jnp.broadcast_to(jnp.exp(-before_me[...]), (PACK, paths))
        upper = earlier.astype(bf16).astype(f32)
        at = lax.broadcasted_iota(jnp.int32, (PACK, paths), 0)
        erow[...] = jnp.where(at == 0, upper, jnp.where(at == 1, earlier - upper, 0.0)).astype(bf16)

    combine(own_chips[0])

    def limb(unit, t, part):
        block = limbs[part, pl.ds((unit * row_tiles + t) * TILE, TILE), :]
        pltpu.matmul_push_rhs(block, staging_register=part, mxu_index=unit)

    row_tiles = paths // TILE // 2
    @pl.when(leads)
    def _():
        for unit in range(2):
            for part in range(2):
                limb(unit, 0, part)
        for t in range(row_tiles):
            for unit in range(2):
                if t > 0:
                    limb(unit, t, 0)
                    limb(unit, t, 1)
                begin = (unit * row_tiles + t) * TILE
                for part in range(2):
                    pltpu.matmul_acc_lhs(totals[4 + unit], erow[:, pl.ds(begin, TILE)], load_staged_rhs=part)
        both = pltpu.matmul_pop(totals[4]) + pltpu.matmul_pop(totals[5])
        line = (both[0:1] + both[1:2]) * (1.0 / (paths * n_path))
        for h in range(SETS // LANES):
            row_a[h] = line[:, h * LANES : (h + 1) * LANES]
        for z in range(n_path - 1):
            @pl.when(z < path_at)
            def _():
                for k in range(n_tm):
                    set_row(z, k).start()
        for other in peers:
            set_row(path_at, other).start()

        for q in other_chips:
            block_copy(q, chip).start()
        from_chips(2, chips - 1 - chip)
        row_copy(hbuf, hbuf, 0, partner).start()
        @pl.when(path_at < n_path - 1)
        def _():
            pl.semaphore_wait(above, n_path - 1 - path_at)
        for z in range(1, n_path):
            @pl.when(z > path_at)
            def _():
                for k in range(n_tm):
                    set_row(z, k).start()
        rows_a[slot] = row_a[lax.div(flat * share, LANES)]

    @pl.when(jnp.logical_not(leads))
    def _():
        hazards(chips, 0).wait_recv()
    before = jnp.zeros((1, paths), f32)
    prefix = []
    for k in range(chips):
        prefix.append(before)
        before = before + hbuf[k]
    if chips < 8:
        prefix.append(jnp.zeros((8 - chips, paths), f32))
    ecol[...] = jnp.transpose(jnp.exp(-jnp.concatenate(prefix, axis=0)))
    factor = ecol[own_rows(me), :]
    recv[chip] = comb[own_rows(me), :]

    span = recv.at[pl.ds(0, chips - 1)]
    blocks = remote(span, span, b_send, b_recv, (path_at, partner))
    blocks.wait_recv()
    result = None
    for k in range(chips):
        term = factor[:, k : k + 1] * recv[k]
        result = term if result is None else result + term
    out[...] = result

    @pl.when(leads)
    def _():
        set_rows(senders - 1).wait_recv()

    @pl.when(jnp.logical_not(leads))
    def _():
        set_rows(senders).wait_recv()
    sums = jnp.sum(rows_a[...], axis=0)
    shift = lax.rem(flat * share, LANES)

    @pl.when(shift == 0)
    def _():
        set_out[...] = sums[:, :share]

    @pl.when(shift != 0)
    def _():
        turned = pltpu.roll(jnp.broadcast_to(sums, (8, LANES)), lax.rem(LANES - shift, LANES), 1)
        set_out[...] = turned[:1, :share]

    blocks.wait_send()

    @pl.when(leads)
    def _():
        hazards(chips, 0).wait_send()
        hazards(chips - 1, 0).wait_send()
        span = rows_a.at[pl.ds(0, senders - 1)]
        sent = remote(span, span, a_send, a_recv, (path_at, partner))
        sent.wait_send()
        span = rows_a.at[pl.ds(0, senders)]
        sent = remote(span, span, a_send, a_recv, (path_at, partner))
        sent.wait_send()
        span = theirs.at[pl.ds(0, paths // 2)]
        remote(span, span, p_send, p_recv.at[0], (path_at, partner)).wait_send()

    @pl.when(jnp.logical_not(leads))
    def _():
        row_copy(bsum, mate_sum, 0, partner).wait_send()
        remote(theirs, theirs, p_send, p_recv.at[0], (path_at, partner)).wait_send()


def finish(pathwise, sets, pathwise_out, sets_out, sem):
    copies = [
        pltpu.make_async_copy(pathwise, pathwise_out, sem.at[0]),
        pltpu.make_async_copy(sets, sets_out, sem.at[1]),
    ]
    for copy in copies:
        copy.start()
    for copy in copies:
        copy.wait()


def solution(mesh):
    n_path, n_tm = mesh.shape["path"], mesh.shape["tm"]
    n_all = n_path * n_tm

    def on_device(values, hazard, spread, trade_set):
        paths, dates, trades = values.shape
        own = paths // n_tm
        chunks = paths // CHUNK_PATHS
        f32 = jnp.float32
        hbm = pl.BlockSpec(memory_space=pltpu.HBM)
        vmem = pl.BlockSpec(memory_space=pltpu.VMEM)
        dma = pltpu.SemaphoreType.DMA
        pathwise, sets = pl.pallas_call(
            functools.partial(kernel, n_path, n_tm),
            out_shape=(pltpu.VMEM((own, SETS), f32), pltpu.VMEM((1, SETS // n_all), f32)),
            in_specs=[hbm, hbm, hbm, hbm],
            out_specs=(vmem, vmem),
            scratch_shapes=[
                pltpu.VMEM((paths * dates, trades), jnp.bfloat16),
                pltpu.VMEM((trades // LANES, LANES), jnp.int32),
                pltpu.VMEM((SETS, trades), jnp.float8_e4m3fn),
                pltpu.VMEM((dates, paths), f32),
                pltpu.SMEM((dates,), f32),
                pltpu.VMEM((chunks, SETS // LANES, CHUNK_PATHS * dates, LANES), f32),
                pltpu.VMEM((paths, 8), f32),
                pltpu.VMEM((paths, SETS), f32),
                pltpu.VMEM((paths, SETS), f32),
                pltpu.VMEM((paths, SETS), f32),
                pltpu.VMEM((n_tm // 2, own, SETS), f32),
                pltpu.VMEM((1, paths), f32),
                pltpu.VMEM((1, paths), f32),
                pltpu.VMEM((1, paths), f32),
                pltpu.VMEM((PACK, paths), jnp.bfloat16),
                pltpu.VMEM((n_tm // 2, 1, paths), f32),
                pltpu.VMEM((paths, 8), f32),
                pltpu.VMEM((paths, max(8, n_tm // 2)), f32),
                pltpu.VMEM((2, paths, SETS), jnp.bfloat16),
                pltpu.VMEM((SETS // LANES, 1, LANES), f32),
                pltpu.VMEM((n_all // 2, 1, LANES), f32),
                dma((2 * chunks,)),
                dma((3,)),
                dma((3,)),
                dma((n_tm // 2,)),
                dma,
                dma,
                pltpu.SemaphoreType.REGULAR,
                pltpu.SemaphoreType.REGULAR,
                pltpu.SemaphoreType.REGULAR,
            ],
            compiler_params=pltpu.CompilerParams(
                collective_id=0, has_side_effects=True, vmem_limit_bytes=62 * 1024 * 1024
            ),
        )(values, hazard, spread, trade_set.reshape(trades // LANES, LANES))
        pathwise = pltpu.with_memory_space_constraint(pathwise, pltpu.VMEM)
        sets = pltpu.with_memory_space_constraint(sets, pltpu.VMEM)
        pathwise, sets = pl.pallas_call(
            finish,
            out_shape=(
                jax.ShapeDtypeStruct(pathwise.shape, f32),
                jax.ShapeDtypeStruct(sets.shape, f32),
            ),
            in_specs=[vmem, vmem],
            out_specs=(hbm, hbm),
            scratch_shapes=[dma((2,))],
        )(pathwise, sets)
        return pathwise, sets.reshape(SETS // n_all)

    in_specs = (P("path", "tm", None), P("tm", "path"), P("tm"), P())
    out_specs = (P(("path", "tm"), None), P(("path", "tm")))
    return jax.shard_map(
        on_device, mesh=mesh, in_specs=in_specs, out_specs=out_specs, check_vma=False
    )
```

```python
import functools

import jax
import jax.numpy as jnp
from jax import lax
from jax.experimental import pallas as pl
from jax.experimental.pallas import tpu as pltpu
from jax.sharding import PartitionSpec as P

SETS = 256
CHUNK_PATHS = 128
LANES = 128
PACK = 16
TILE = 256
BARRIER_AFTER = 1
MESH = pl.DeviceIdType.MESH


def kernel(n_path, n_tm, *refs):
    rows = CHUNK_PATHS * refs[0].shape[1]
    sums = [pltpu.ACC(unit)((rows, SETS), jnp.float32) for unit in (0, 0, 1, 1)]
    sums += [pltpu.ACC(unit)((PACK, SETS), jnp.float32) for unit in (0, 1)]
    sums += [pltpu.ACC(unit)((rows // 2, SETS), jnp.float32) for unit in (0, 0, 1, 1)]
    pl.run_scoped(lambda *totals: body(n_path, n_tm, totals, *refs), *sums)


def body(
    n_path, n_tm, totals, values, hazard_in, spread_in, trade_in, out, set_out,
    vbuf, ts, oh, hz, spread, nbuf, wt, contrib, theirs, comb, recv, bsum, mate_sum, before_me, erow, hbuf, pcol, ecol, limbs, row_a, rows_a,
    load_sem, small_sem, h_recv, p_recv, b_recv, a_recv, mate, ready, above,
):
    paths, dates, trades = values.shape
    f32, bf16 = jnp.float32, jnp.bfloat16
    own = paths // n_tm
    chunks = paths // CHUNK_PATHS
    per = n_tm // chunks
    n_all = n_path * n_tm
    chips = n_tm // 2
    share = SETS // n_all
    path_at, me = lax.axis_index("path"), lax.axis_index("tm")
    flat = path_at * n_tm + me
    chip, core = lax.div(me, 2), lax.rem(me, 2)
    partner = me + 1 - 2 * core
    peers = [lax.rem(me + k, n_tm) for k in range(1, n_tm)]
    leads = core == 1
    lead_peers = [lax.rem(chip + k, chips) * 2 + 1 for k in range(1, chips)]
    senders = n_path * chips
    slot = path_at * chips + chip
    rows = CHUNK_PATHS * dates
    my_chunk = lax.div(me, per)
    if chunks == 4:
        high, low = lax.div(my_chunk, 2), lax.rem(my_chunk, 2)
        first = [2 * (1 - high) + 1 - low, 2 * high + 1 - low, 2 * (1 - high) + low, my_chunk]
    else:
        first = [lax.rem(my_chunk + 1 + i, chunks) for i in range(chunks)]
    flat_values = values.reshape(paths * dates, trades)

    last = chunks - 1
    h_send, p_send, b_send, a_send = small_sem.at[0], load_sem.at[0], load_sem.at[1], load_sem.at[2]

    def load(i, part):
        begin = pl.multiple_of(first[i] * rows, rows)
        if i == last:
            area = (pl.ds(pl.multiple_of(begin + part * rows // 2, rows // 2), rows // 2), slice(None))
        else:
            area = (pl.ds(begin, rows), pl.ds(part * trades // 2, trades // 2))
        return pltpu.make_async_copy(flat_values.at[area], vbuf.at[area], load_sem.at[2 * i + part])

    barrier = pltpu.get_barrier_semaphore()
    pl.semaphore_signal(barrier, inc=1, device_id=(path_at, partner), device_id_type=MESH)

    @pl.when(leads)
    def _():
        for other in lead_peers:
            pl.semaphore_signal(barrier, inc=1, device_id=(path_at, other), device_id_type=MESH)

    copy_hazard = pltpu.make_async_copy(hazard_in, hz, small_sem.at[0])
    copy_trades = pltpu.make_async_copy(trade_in, ts, small_sem.at[1])
    copy_spread = pltpu.make_async_copy(spread_in, spread, small_sem.at[2])
    copy_hazard.start()
    copy_trades.start()
    copy_spread.start()
    for i in range(chunks):
        for part in range(2):
            load(i, part).start()
    for z in range(1, n_path):
        @pl.when(z > path_at)
        def _():
            pl.semaphore_signal(barrier, inc=1, device_id=(z, me), device_id_type=MESH)

    def remote(src, dst, send, recv_at, device):
        return pltpu.make_async_remote_copy(
            src_ref=src, dst_ref=dst, send_sem=send, recv_sem=recv_at, device_id=device, device_id_type=MESH
        )

    def chunk_span(i):
        return pl.ds(pl.multiple_of(first[i] * CHUNK_PATHS, CHUNK_PATHS), CHUNK_PATHS)

    def own_rows(index):
        return pl.ds(pl.multiple_of(index * own, own), own)

    def row_copy(src, dst, arrival, other):
        return remote(src, dst, h_send, h_recv.at[arrival], (path_at, other))

    def hazards(count, arrival):
        span = hbuf.at[pl.ds(0, count)]
        return remote(span, span, h_send, h_recv.at[arrival], (path_at, partner))

    def from_chips(arrival, chips_there):
        for c in range(1, chips):
            @pl.when(chips_there == c)
            def _():
                hazards(c, arrival).wait_recv()

    def both_rows(q):
        return pl.ds(pl.multiple_of(q * 2 * own, 2 * own), 2 * own)

    def pair_copy(q, span):
        return remote(contrib.at[span], theirs.at[span], p_send, p_recv.at[q], (path_at, partner))

    def per_core(q, act):
        @pl.when(leads)
        def _():
            act(q, own_rows(q * 2), both_rows(q))

        @pl.when(jnp.logical_not(leads))
        def _():
            act(q, both_rows(q), own_rows(q * 2))

    def block_copy(q, slot_at):
        return remote(comb.at[own_rows(q * 2 + core)], recv.at[slot_at], b_send, b_recv, (path_at, q * 2 + core))

    def set_row(z, other):
        piece = lax.div((z * n_tm + other) * share, LANES)
        return remote(row_a.at[piece], rows_a.at[slot], a_send, a_recv, (z, other))

    def set_rows(count):
        span = rows_a.at[pl.ds(0, count)]
        return remote(span, span, a_send, a_recv, (path_at, partner))

    copy_hazard.wait()
    bsum[...] = sum(hz[pl.ds(d, 1), :] for d in range(dates))

    def meet():
        pl.semaphore_wait(barrier, 1 + path_at + core * (chips - 1))

        @pl.when(jnp.logical_not(leads))
        def _():
            row_copy(bsum, mate_sum, 0, partner).start()
            pl.semaphore_signal(mate, inc=1, device_id=(path_at, partner), device_id_type=MESH)

        @pl.when(leads)
        def _():
            pl.semaphore_wait(mate, 1)
            for other in lead_peers:
                pl.semaphore_signal(ready, inc=1, device_id=(path_at, other), device_id_type=MESH)
            row_copy(bsum, mate_sum, 0, partner).wait_recv()
            hbuf[chip] = bsum[...] + mate_sum[...]
            for k in range(1, chips):
                there = lax.rem(chip + k, chips)
                row_copy(hbuf.at[chip], hbuf.at[chip], jnp.where(there > chip, 1, 2), there * 2 + 1).start()

    @pl.when(jnp.logical_not(leads))
    def _():
        meet()
    copy_trades.wait()
    base = lax.broadcasted_iota(jnp.int32, (PACK, LANES), 0)
    set_at = [(base + PACK * r).astype(f32).astype(bf16) for r in range(SETS // PACK)]
    one, zero = jnp.ones((PACK, LANES), bf16), jnp.zeros((PACK, LANES), bf16)
    for block in range(trades // LANES):
        ids = jnp.broadcast_to(ts[pl.ds(block, 1), :], (PACK, LANES)).astype(f32).astype(bf16)
        for r in range(SETS // PACK):
            picked = jnp.where(ids == set_at[r], one, zero)
            oh[pl.ds(r * PACK, PACK), pl.ds(block * LANES, LANES)] = picked.astype(oh.dtype)

    copy_spread.wait()
    total = jnp.zeros((1, paths), f32)
    weight_rows = []
    scale = 1.0 / (dates * n_tm)
    for d in range(dates):
        total = total + hz[pl.ds(d, 1), :]
        weight_rows.append((spread[d] * scale) * jnp.exp(-total))
    weight_rows.append(jnp.zeros((8 - dates, paths), f32))
    wt[...] = jnp.transpose(jnp.concatenate(weight_rows, axis=0))

    def exchange(i):
        for k in range(per // 2):
            per_core(first[i] * (per // 2) + k, lambda q, send, take: pair_copy(q, send).start())

    def exchange_half(part):
        chips_here = per // 2
        if chips_here > 1:
            for k in range(part * chips_here // 2, (part + 1) * chips_here // 2):
                per_core(first[last] * chips_here + k, lambda q, send, take: pair_copy(q, send).start())
            return

        @pl.when(jnp.logical_not(leads))
        def _():
            pair_copy(my_chunk, own_rows(my_chunk * 2 + part)).start()

        if part == 0:
            @pl.when(leads)
            def _():
                pair_copy(my_chunk, own_rows(my_chunk * 2)).start()

    def combine(q):
        @pl.when(leads)
        def _():
            span = both_rows(q)
            comb[span, :] = pcol[span, 0:1] * contrib[span, :]

        per_core(q, lambda q, send, take: pair_copy(q, take).wait_recv())

        @pl.when(leads)
        def _():
            span = both_rows(q)
            both = theirs[span, :] + comb[span, :]
            comb[span, :] = both
            upper = both.astype(bf16)
            limbs[0, span, :] = upper
            limbs[1, span, :] = (both - upper.astype(f32)).astype(bf16)

        @pl.when(jnp.logical_not(leads))
        def _():
            span = own_rows(q * 2)
            comb[span, :] = contrib[span, :] + pcol[span, 0:1] * theirs[span, :]

    own_chips = [my_chunk * (per // 2) + lax.rem(lax.rem(chip, per // 2) + k, per // 2) for k in range(per // 2)]
    other_chips = [first[i] * (per // 2) + k for i in range(chunks - 1) for k in range(per // 2)]
    other_chips += own_chips[1:]

    tiles = trades // TILE // 2

    def push(n):
        for unit in range(2):
            ids = oh[:, pl.ds((2 * (n % tiles) + unit) * TILE, TILE)]
            pltpu.matmul_push_rhs(ids, staging_register=n % 2, mxu_index=unit, transpose=True)

    def multiply(n, span, into, steps):
        for t in steps:
            if n + t + 1 < (chunks + 1) * tiles:
                push(n + t + 1)
            for unit in range(2):
                block = vbuf[span, pl.ds((2 * t + unit) * TILE, TILE)]
                pltpu.matmul_acc_lhs(into[unit], block, load_staged_rhs=(n + t) % 2)

    def weigh(i, begin, paths_here, done):
        netted = pltpu.matmul_pop(done[0]) + pltpu.matmul_pop(done[1])
        for h in range(SETS // LANES):
            nbuf[i, h, pl.ds(begin * dates, paths_here * dates)] = netted[:, h * LANES : (h + 1) * LANES]
        path_span = pl.ds(pl.multiple_of(first[i] * CHUNK_PATHS + begin, paths_here), paths_here)
        weight = wt[path_span, :]
        for h in range(SETS // LANES):
            part = None
            for d in range(dates):
                picked = nbuf[i, h, pl.ds(begin * dates + d, paths_here, stride=dates), :]
                term = weight[:, d : d + 1] * jnp.maximum(picked, 0.0)
                part = term if part is None else part + term
            contrib[path_span, pl.ds(h * LANES, LANES)] = part

    def whole(i):
        return totals[i % 2], totals[2 + i % 2]

    def in_half(part):
        return totals[6 + part], totals[8 + part]

    some = CHUNK_PATHS // 2
    push(0)
    for i in range(chunks):
        for part in range(2):
            load(i, part).wait()
            if part == 0 and i > 0:
                weigh(i - 1, 0, CHUNK_PATHS, whole(i - 1))
            if i < last:
                span = pl.ds(pl.multiple_of(first[i] * rows, rows), rows)
                steps = range(part * tiles // 2, (part + 1) * tiles // 2)
                multiply(i * tiles, span, whole(i), steps)
            else:
                if part == 1:
                    weigh(i, 0, some, in_half(0))
                begin = pl.multiple_of(first[i] * rows + part * rows // 2, rows // 2)
                multiply((i + part) * tiles, pl.ds(begin, rows // 2), in_half(part), range(tiles))
            if i == BARRIER_AFTER and part == 1:
                @pl.when(leads)
                def _():
                    meet()
            if i == last:
                if part == 0:
                    exchange(last - 1)
                else:
                    exchange_half(0)
            elif part == 1 and i > 0 and i >= BARRIER_AFTER:
                for j in range(0 if i == max(BARRIER_AFTER, 1) else i - 1, i):
                    exchange(j)
    weigh(last, some, some, in_half(1))
    exchange_half(1)

    @pl.when(jnp.logical_not(leads))
    def _():
        mate_sum[...] = bsum[...]
    pcol[...] = jnp.transpose(jnp.broadcast_to(jnp.exp(-mate_sum[...]), (8, paths)))
    @pl.when(leads)
    def _():
        pl.semaphore_wait(ready, chips - 1)
        pl.semaphore_signal(mate, inc=1, device_id=(path_at, partner), device_id_type=MESH)
        for z in range(n_path - 1):
            @pl.when(z < path_at)
            def _():
                pl.semaphore_signal(above, inc=1, device_id=(z, me), device_id_type=MESH)

    @pl.when(jnp.logical_not(leads))
    def _():
        combine(other_chips[0])
        pl.semaphore_wait(mate, 1)
        block_copy(other_chips[0], chip).start()

    @pl.when(leads)
    def _():
        combine(other_chips[0])

    for q in other_chips[1:]:
        combine(q)

        @pl.when(jnp.logical_not(leads))
        def _():
            block_copy(q, chip).start()

    @pl.when(leads)
    def _():
        from_chips(1, chip)
        before_me[...] = jnp.zeros((1, paths), f32)
        for c in range(1, chips):
            @pl.when(chip == c)
            def _():
                before_me[...] = sum(hbuf[k] for k in range(c))
        earlier = jnp.broadcast_to(jnp.exp(-before_me[...]), (PACK, paths))
        upper = earlier.astype(bf16).astype(f32)
        at = lax.broadcasted_iota(jnp.int32, (PACK, paths), 0)
        erow[...] = jnp.where(at == 0, upper, jnp.where(at == 1, earlier - upper, 0.0)).astype(bf16)

    combine(own_chips[0])

    def limb(unit, t, part):
        block = limbs[part, pl.ds((unit * row_tiles + t) * TILE, TILE), :]
        pltpu.matmul_push_rhs(block, staging_register=part, mxu_index=unit)

    row_tiles = paths // TILE // 2
    @pl.when(leads)
    def _():
        for unit in range(2):
            for part in range(2):
                limb(unit, 0, part)
        for t in range(row_tiles):
            for unit in range(2):
                if t > 0:
                    limb(unit, t, 0)
                    limb(unit, t, 1)
                begin = (unit * row_tiles + t) * TILE
                for part in range(2):
                    pltpu.matmul_acc_lhs(totals[4 + unit], erow[:, pl.ds(begin, TILE)], load_staged_rhs=part)
        both = pltpu.matmul_pop(totals[4]) + pltpu.matmul_pop(totals[5])
        line = (both[0:1] + both[1:2]) * (1.0 / (paths * n_path))
        for h in range(SETS // LANES):
            row_a[h] = line[:, h * LANES : (h + 1) * LANES]
        for z in range(n_path - 1):
            @pl.when(z < path_at)
            def _():
                for k in range(n_tm):
                    set_row(z, k).start()
        for other in peers:
            set_row(path_at, other).start()

        for q in other_chips:
            block_copy(q, chip).start()
        from_chips(2, chips - 1 - chip)
        row_copy(hbuf, hbuf, 0, partner).start()
        @pl.when(path_at < n_path - 1)
        def _():
            pl.semaphore_wait(above, n_path - 1 - path_at)
        for z in range(1, n_path):
            @pl.when(z > path_at)
            def _():
                for k in range(n_tm):
                    set_row(z, k).start()
        rows_a[slot] = row_a[lax.div(flat * share, LANES)]

    @pl.when(jnp.logical_not(leads))
    def _():
        hazards(chips, 0).wait_recv()
    before = jnp.zeros((1, paths), f32)
    prefix = []
    for k in range(chips):
        prefix.append(before)
        before = before + hbuf[k]
    if chips < 8:
        prefix.append(jnp.zeros((8 - chips, paths), f32))
    ecol[...] = jnp.transpose(jnp.exp(-jnp.concatenate(prefix, axis=0)))
    factor = ecol[own_rows(me), :]
    recv[chip] = comb[own_rows(me), :]

    span = recv.at[pl.ds(0, chips - 1)]
    blocks = remote(span, span, b_send, b_recv, (path_at, partner))
    blocks.wait_recv()
    result = None
    for k in range(chips):
        term = factor[:, k : k + 1] * recv[k]
        result = term if result is None else result + term
    out[...] = result

    @pl.when(leads)
    def _():
        set_rows(senders - 1).wait_recv()

    @pl.when(jnp.logical_not(leads))
    def _():
        set_rows(senders).wait_recv()
    sums = jnp.sum(rows_a[...], axis=0)
    shift = lax.rem(flat * share, LANES)

    @pl.when(shift == 0)
    def _():
        set_out[...] = sums[:, :share]

    @pl.when(shift != 0)
    def _():
        turned = pltpu.roll(jnp.broadcast_to(sums, (8, LANES)), lax.rem(LANES - shift, LANES), 1)
        set_out[...] = turned[:1, :share]

    blocks.wait_send()

    @pl.when(leads)
    def _():
        hazards(chips, 0).wait_send()
        hazards(chips - 1, 0).wait_send()
        span = rows_a.at[pl.ds(0, senders - 1)]
        sent = remote(span, span, a_send, a_recv, (path_at, partner))
        sent.wait_send()
        span = rows_a.at[pl.ds(0, senders)]
        sent = remote(span, span, a_send, a_recv, (path_at, partner))
        sent.wait_send()
        span = theirs.at[pl.ds(0, paths // 2)]
        remote(span, span, p_send, p_recv.at[0], (path_at, partner)).wait_send()

    @pl.when(jnp.logical_not(leads))
    def _():
        row_copy(bsum, mate_sum, 0, partner).wait_send()
        remote(theirs, theirs, p_send, p_recv.at[0], (path_at, partner)).wait_send()


def finish(pathwise, sets, pathwise_out, sets_out, sem):
    copies = [
        pltpu.make_async_copy(pathwise, pathwise_out, sem.at[0]),
        pltpu.make_async_copy(sets, sets_out, sem.at[1]),
    ]
    for copy in copies:
        copy.start()
    for copy in copies:
        copy.wait()


def solution(mesh):
    n_path, n_tm = mesh.shape["path"], mesh.shape["tm"]
    n_all = n_path * n_tm

    def on_device(values, hazard, spread, trade_set):
        paths, dates, trades = values.shape
        own = paths // n_tm
        chunks = paths // CHUNK_PATHS
        f32 = jnp.float32
        hbm = pl.BlockSpec(memory_space=pltpu.HBM)
        vmem = pl.BlockSpec(memory_space=pltpu.VMEM)
        dma = pltpu.SemaphoreType.DMA
        pathwise, sets = pl.pallas_call(
            functools.partial(kernel, n_path, n_tm),
            out_shape=(pltpu.VMEM((own, SETS), f32), pltpu.VMEM((1, SETS // n_all), f32)),
            in_specs=[hbm, hbm, hbm, hbm],
            out_specs=(vmem, vmem),
            scratch_shapes=[
                pltpu.VMEM((paths * dates, trades), jnp.bfloat16),
                pltpu.VMEM((trades // LANES, LANES), jnp.int32),
                pltpu.VMEM((SETS, trades), jnp.float8_e4m3fn),
                pltpu.VMEM((dates, paths), f32),
                pltpu.SMEM((dates,), f32),
                pltpu.VMEM((chunks, SETS // LANES, CHUNK_PATHS * dates, LANES), f32),
                pltpu.VMEM((paths, 8), f32),
                pltpu.VMEM((paths, SETS), f32),
                pltpu.VMEM((paths, SETS), f32),
                pltpu.VMEM((paths, SETS), f32),
                pltpu.VMEM((n_tm // 2, own, SETS), f32),
                pltpu.VMEM((1, paths), f32),
                pltpu.VMEM((1, paths), f32),
                pltpu.VMEM((1, paths), f32),
                pltpu.VMEM((PACK, paths), jnp.bfloat16),
                pltpu.VMEM((n_tm // 2, 1, paths), f32),
                pltpu.VMEM((paths, 8), f32),
                pltpu.VMEM((paths, max(8, n_tm // 2)), f32),
                pltpu.VMEM((2, paths, SETS), jnp.bfloat16),
                pltpu.VMEM((SETS // LANES, 1, LANES), f32),
                pltpu.VMEM((n_all // 2, 1, LANES), f32),
                dma((2 * chunks,)),
                dma((3,)),
                dma((3,)),
                dma((n_tm // 2,)),
                dma,
                dma,
                pltpu.SemaphoreType.REGULAR,
                pltpu.SemaphoreType.REGULAR,
                pltpu.SemaphoreType.REGULAR,
            ],
            compiler_params=pltpu.CompilerParams(
                collective_id=0, has_side_effects=True, vmem_limit_bytes=62 * 1024 * 1024
            ),
        )(values, hazard, spread, trade_set.reshape(trades // LANES, LANES))
        pathwise = pltpu.with_memory_space_constraint(pathwise, pltpu.VMEM)
        sets = pltpu.with_memory_space_constraint(sets, pltpu.VMEM)
        pathwise, sets = pl.pallas_call(
            finish,
            out_shape=(
                jax.ShapeDtypeStruct(pathwise.shape, f32),
                jax.ShapeDtypeStruct(sets.shape, f32),
            ),
            in_specs=[vmem, vmem],
            out_specs=(hbm, hbm),
            scratch_shapes=[dma((2,))],
        )(pathwise, sets)
        return pathwise, sets.reshape(SETS // n_all)

    in_specs = (P("path", "tm", None), P("tm", "path"), P("tm"), P())
    out_specs = (P(("path", "tm"), None), P(("path", "tm")))
    return jax.shard_map(
        on_device, mesh=mesh, in_specs=in_specs, out_specs=out_specs, check_vma=False
    )
```
